32 devices in a mesh: zero: 8 (over y, x, core), width: 4 (over z).
Axes of the slice: x: 2, y: 2, z: 4, core: 2. Of those that a mesh axis runs over, the one named last changes fastest.
Arguments:
- train_query: bfloat16 [3584, 4096], P('zero', 'width'), may hold values from -0.09375 to 0.09375
- low_query: bfloat16 [3584, 32], P('zero'), may hold values from -0.09375 to 0.09375
- high_query: bfloat16 [32, 4096], P(None, 'width'), may hold values from -1 to 1
- train_key: bfloat16 [3584, 2048], P('zero', 'width'), may hold values from -0.09375 to 0.09375
- low_key: bfloat16 [3584, 32], P('zero'), may hold values from -0.09375 to 0.09375
- high_key: bfloat16 [32, 2048], P(None, 'width'), may hold values from -1 to 1
- train_value: bfloat16 [3584, 2048], P('zero', 'width'), may hold values from -0.09375 to 0.09375
- low_value: bfloat16 [3584, 32], P('zero'), may hold values from -0.09375 to 0.09375
- high_value: bfloat16 [32, 2048], P(None, 'width'), may hold values from -1 to 1
- train_mixed: bfloat16 [4096, 3584], P('width', 'zero'), may hold values from -0.09375 to 0.09375
- low_mixed: bfloat16 [4096, 32], P('width'), may hold values from -0.09375 to 0.09375
- high_mixed: bfloat16 [32, 3584], P(None, 'zero'), may hold values from -1 to 1
- norm_train: float32 [3584], P(('zero', 'width')), may hold values from 0.25 to 1.75
- norm_step: float32 [3584], P(('zero', 'width')), may hold values from -0.3 to 0.3
Outputs:
- ready_query: bfloat16 [4096, 3584], P('width')
- ready_key: bfloat16 [2048, 3584], P('width')
- ready_value: bfloat16 [2048, 3584], P('width')
- ready_mixed: bfloat16 [3584, 4096], P(None, 'width')
- serve_norm: bfloat16 [3584], replicated
The draws below stay inside these ranges and needn't reach their ends.
All inputs are finite; a program needn't handle non-finite values.
Results may differ from the reference program's by a relative error of at most 0.001.
Values may be sent and summed in bfloat16 or wider, within the bound.
A program may use at most 128 MiB of HBM per device.

```python
import jax
import jax.numpy as jnp

D_MODEL = 3584
Q_DIM = 4096
KV_DIM = 2048
RANK = 32


def level_of(rng, extent, cuts, least, high):
    def one(dim, blocks):
        draws = jax.random.uniform(jax.random.fold_in(jax.random.fold_in(rng, 6), dim), (blocks,), jnp.float32, least / len(cuts), high / len(cuts))
        return jnp.repeat(jnp.exp(draws), extent[dim] // blocks).reshape((-1,) + (1,) * (len(extent) - dim - 1))

    gain = one(*cuts[0])
    for cut in cuts[1:]:
        gain = gain * one(*cut)
    return gain


def normal_values(own_key, extent, spread, most, cuts=(), held_as=jnp.bfloat16):
    drawn = jax.random.normal(own_key, extent, jnp.float32) * spread
    if len(cuts) > 0:
        drawn = level_of(own_key, extent, cuts, -0.22, 0.18) * drawn
    return jnp.clip(drawn, min=-most, max=most).astype(held_as)


def setup_inputs(seed: int = 0) -> dict:
    seeds = jax.random.split(jax.random.key(seed), 15)
    return {
        "train_query": normal_values(seeds[0], (D_MODEL, Q_DIM), D_MODEL ** -0.5, 0.09375, ((0, 8), (1, 4))),
        "low_query": normal_values(seeds[1], (D_MODEL, RANK), D_MODEL ** -0.5, 0.09375, ((0, 8),)),
        "high_query": normal_values(seeds[2], (RANK, Q_DIM), RANK ** -0.5, 1.0, ((1, 4),)),
        "train_key": normal_values(seeds[3], (D_MODEL, KV_DIM), D_MODEL ** -0.5, 0.09375, ((0, 8), (1, 4))),
        "low_key": normal_values(seeds[4], (D_MODEL, RANK), D_MODEL ** -0.5, 0.09375, ((0, 8),)),
        "high_key": normal_values(seeds[5], (RANK, KV_DIM), RANK ** -0.5, 1.0, ((1, 4),)),
        "train_value": normal_values(seeds[6], (D_MODEL, KV_DIM), D_MODEL ** -0.5, 0.09375, ((0, 8), (1, 4))),
        "low_value": normal_values(seeds[7], (D_MODEL, RANK), D_MODEL ** -0.5, 0.09375, ((0, 8),)),
        "high_value": normal_values(seeds[8], (RANK, KV_DIM), RANK ** -0.5, 1.0, ((1, 4),)),
        "train_mixed": normal_values(seeds[9], (Q_DIM, D_MODEL), Q_DIM ** -0.5, 0.09375, ((0, 4), (1, 8))),
        "low_mixed": normal_values(seeds[10], (Q_DIM, RANK), Q_DIM ** -0.5, 0.09375, ((0, 4),)),
        "high_mixed": normal_values(seeds[11], (RANK, D_MODEL), RANK ** -0.5, 1.0, ((1, 8),)),
        "norm_train": jnp.clip(1.0 + 0.15 * jax.random.normal(seeds[12], (D_MODEL,), jnp.float32), 0.25, 1.75),
        "norm_step": jnp.clip(jax.random.uniform(seeds[13], (D_MODEL,), jnp.float32, -0.3, 0.3) * level_of(seeds[13], (D_MODEL,), ((0, 32),), -0.4, 0.0), -0.3, 0.3),
    }


mix_rate = 0.5


def reference(train_query, low_query, high_query, train_key, low_key, high_key, train_value, low_value, high_value, train_mixed, low_mixed, high_mixed, norm_train, norm_step):
    latest_query = train_query.astype(jnp.float32) + mix_rate * jnp.dot(low_query, high_query, preferred_element_type=jnp.float32)
    latest_key = train_key.astype(jnp.float32) + mix_rate * jnp.dot(low_key, high_key, preferred_element_type=jnp.float32)
    latest_value = train_value.astype(jnp.float32) + mix_rate * jnp.dot(low_value, high_value, preferred_element_type=jnp.float32)
    latest_mixed = train_mixed.astype(jnp.float32) + mix_rate * jnp.dot(low_mixed, high_mixed, preferred_element_type=jnp.float32)
    ready_query = latest_query.T.astype(jnp.bfloat16)
    ready_key = latest_key.T.astype(jnp.bfloat16)
    ready_value = latest_value.T.astype(jnp.bfloat16)
    ready_mixed = latest_mixed.T.astype(jnp.bfloat16)
    serve_norm = (norm_train + norm_step).astype(jnp.bfloat16)
    return ready_query, ready_key, ready_value, ready_mixed, serve_norm
```

```python
import functools
import math

import jax
import jax.numpy as jnp
from jax import lax
from jax.experimental import pallas as pl
from jax.experimental.pallas import tpu as pltpu
from jax.sharding import PartitionSpec as P

mix_rate = 0.5
CORES = 2
LANES = 128
F32 = jnp.float32
BF16 = jnp.bfloat16
EARLY = 5
VMEM_BYTES = 67_043_328
VMEM = pltpu.VMEM
HBM = pltpu.MemorySpace.HBM
TO_X, TO_Y, ON, P_OWN, P_X, P_Y = range(6)


def plain_body(
    train_query, low_query, high_query, train_key, low_key, high_key, train_value, low_value, high_value,
    train_mixed, low_mixed, high_mixed, norm_train, norm_step,
):
    def merged(train, low, high):
        return (train.astype(F32) + mix_rate * jnp.dot(low, high, preferred_element_type=F32)).astype(BF16)

    return (
        lax.all_gather(merged(train_query, low_query, high_query), "zero", axis=0, tiled=True).T,
        lax.all_gather(merged(train_key, low_key, high_key), "zero", axis=0, tiled=True).T,
        lax.all_gather(merged(train_value, low_value, high_value), "zero", axis=0, tiled=True).T,
        lax.all_gather(merged(train_mixed, low_mixed, high_mixed).T, "zero", axis=0, tiled=True),
        lax.all_gather((norm_train + norm_step).astype(BF16), ("zero", "width"), axis=0, tiled=True),
    )


class Place:
    def __init__(self):
        self.me, self.w = lax.axis_index("zero"), lax.axis_index("width")
        me = self.me
        self.c = lax.rem(me, 2)
        x = lax.rem(lax.div(me, 2), 2)
        self.y = lax.div(me, 4)
        self.chip = lax.div(me, 2)
        self.partner, self.xn, self.yn = me + 1 - 2 * self.c, me + 2 - 4 * x, me + 4 - 8 * self.y
        self.chip_x, self.chip_y, self.chip_d = self.chip + 1 - 2 * x, self.chip + 2 - 4 * self.y, 3 - self.chip


def remote(src, dst, ssem, rsem, **where):
    return pltpu.make_async_remote_copy(
        src_ref=src, dst_ref=dst, send_sem=ssem, recv_sem=rsem, device_id=where, device_id_type=pl.DeviceIdType.MESH
    )


def tell(sem, **where):
    pl.semaphore_signal(sem, inc=1, device_id=where, device_id_type=pl.DeviceIdType.MESH)


def unit_list(rows, mix, nq, nk):
    quarter = mix // 4
    parts = ((0, nk // 2), (nk // 2, nk // 4), (nk - nk // 4, nk // 4))
    first = [(3, 0, quarter), (3, quarter, quarter), (0, 0, nq // 4), (0, nq // 4, nq // 4)]
    second = [(3, 2 * quarter, quarter), (3, 3 * quarter, quarter), (0, nq // 2, nq // 4), (0, 3 * nq // 4, nq // 4)]
    return first + [(1, *p) for p in parts] + second + [(2, *p) for p in parts]


def region(unit, outs, rows, chip, c):
    a, start, size = unit
    out = outs[a]
    if a == 3:
        return out.at[pl.ds(pl.multiple_of(rows * (2 * chip + c), 16), rows), start : start + size]
    pair = 2 * rows
    return out.at[
        pl.ds(pl.multiple_of(c * (out.shape[0] // 2) + start, 16), size), pl.ds(pl.multiple_of(pair * chip, LANES), pair)
    ]


def arrived(ref, sem):
    pltpu.make_async_copy(ref, ref, sem).wait()


def gather(
    zeros, widths,
    tq_h, lq_h, hq_h, tk_h, lk_h, hk_h, tv_h, lv_h, hv_h, tm_h, lm_h, hm_h, nt_h, ns_h,
    oq, ok, ov, om, on,
    tm, pair_m, held, lows, highs, gains, own_q, own_k, own_v, own_m, joined,
    fetched, keep, swap_send, swap_recv, send, arrive, across, early_send, early_recv, nsend, nrecv,
):
    at = Place()
    c, chip = at.c, at.chip
    rows = tq_h.shape[0]
    pair = 2 * rows
    mix = tm_h.shape[1]
    quarter = mix // 4
    outs = (oq, ok, ov, om)
    nq, nk = oq.shape[0] // 2, ok.shape[0] // 2
    units = unit_list(rows, mix, nq, nk)
    n = len(units) // 2
    share = om.at[: rows * (mix + 2 * nq + 4 * nk) // mix, :]
    LOW_HIGH, FIRST, OTHERS, GAINS, LOWS, HIGHS, TRAINS = range(7)

    def rank_dot(left, right):
        return lax.dot_general(left, right, (((0,), (0,)), ((), ())), preferred_element_type=F32)

    def fetch(src, dst, sem):
        pltpu.make_async_copy(src, dst, fetched.at[sem]).start()

    fetch(lm_h, pair_m.at[:, :mix], LOW_HIGH)
    fetch(hm_h, pair_m.at[:, mix:], LOW_HIGH)
    fetch(tm_h.at[:, :quarter], tm.at[:, :quarter], FIRST)
    barrier = pltpu.get_barrier_semaphore()
    for other in (at.xn, at.yn, at.partner):
        tell(barrier, zero=other)
    fetch(tm_h.at[:, quarter:], tm.at[:, quarter:], OTHERS)
    fetch(nt_h, gains.at[0], GAINS)
    fetch(ns_h, gains.at[1], GAINS)

    mine = pl.ds(pl.multiple_of(rows * c, 16), rows)
    spans, spot = [], 0
    for train in (tq_h, tk_h, tv_h):
        spans.append(slice(spot, spot + train.shape[1] // 2))
        spot += train.shape[1] // 2
    for k, (train, low, high) in enumerate(((tq_h, lq_h, hq_h), (tk_h, lk_h, hk_h), (tv_h, lv_h, hv_h))):
        half = train.shape[1] // 2
        cols = pl.ds(pl.multiple_of(c * half, LANES), half)
        fetch(train.at[:, cols], held.at[mine, spans[k]], TRAINS)
        fetch(low, lows.at[k, c], LOWS)
        fetch(high, highs.at[:, 2 * spans[k].start : 2 * spans[k].stop], HIGHS)

    def merge_mixed(h):
        cols = slice(h * quarter, (h + 1) * quarter)
        merged = tm[:, cols].astype(F32) + mix_rate * rank_dot(pair_m[:, mix:], pair_m[:, cols])
        own_m[:, cols] = merged.astype(BF16)

    sources = [
        own_m.at[:, s : s + size] if a == 3 else (own_q, own_k, own_v)[a].at[s : s + size, :] for a, s, size in units
    ]

    def move(k, kind):
        p = {ON: at.chip_x if k < n else at.chip_y, P_X: at.chip_x, P_Y: at.chip_y}.get(kind, chip)
        there = region(units[k], outs, rows, p, c)
        where = {TO_X: at.xn, TO_Y: at.yn, ON: at.yn if k < n else at.xn}.get(kind, at.partner)
        if kind in (TO_X, TO_Y):
            recv = arrive.at[k % n + (n if (kind == TO_X) == (k >= n) else 0)]
        elif kind == ON:
            recv = early_recv
        else:
            recv = across.at[kind - P_OWN]
        return remote(
            sources[k] if kind in (TO_X, TO_Y, P_OWN) else there, there,
            early_send if kind == ON else send.at[kind - (kind > ON)], recv, zero=where,
        )

    def come(j, late):
        a, _, size = units[j]
        both = om.at[:rows, : 2 * size] if a == 3 else oq.at[: 2 * size, :pair]
        arrived(both, arrive.at[j + n * late])

    arrived(pair_m, fetched.at[LOW_HIGH])
    arrived(tm.at[:, :quarter], fetched.at[FIRST])
    merge_mixed(0)
    pl.semaphore_wait(barrier, 3)
    move(0, TO_X).start()
    move(0, TO_Y).start()
    arrived(tm.at[:, quarter:], fetched.at[OTHERS])
    merge_mixed(2)
    merge_mixed(1)
    merge_mixed(3)
    move(n, TO_Y).start()
    for j in (1,):
        move(j, TO_X).start()
        move(n + j, TO_Y).start()

    for k, (train, low) in enumerate(((tq_h, lq_h), (tk_h, lk_h), (tv_h, lv_h))):
        half = train.shape[1] // 2
        cols = pl.ds(pl.multiple_of((1 - c) * half, LANES), half)
        remote(train.at[:, cols], held.at[mine, spans[k]], swap_send.at[0], swap_recv.at[0], zero=at.partner).start()
        remote(low, lows.at[k, c], swap_send.at[1], swap_recv.at[1], zero=at.partner).start()

    def keep_own(source, there):
        pltpu.make_async_copy(source, there, keep).start()

    keep_own(own_m, om.at[pl.ds(pl.multiple_of(rows * at.me, 16), rows), :])

    arrived(gains, fetched.at[GAINS])
    on[c, chip] = jnp.pad(gains[0] + gains[1], ((0, 0), (0, LANES - gains.shape[2])))
    row = on.at[c, pl.ds(chip, 1)]
    both_rows = on.at[c, pl.ds(2 * at.y, 2)]
    small = [remote(row, row, nsend.at[0], nrecv.at[0], zero=at.xn)]
    small[0].start()

    def merge(e, out, own_out):
        span = spans[e]
        half = span.stop - span.start
        joined[:, :rows] = lows[e, 0]
        joined[:, rows:] = lows[e, 1]
        cols = pl.ds(pl.multiple_of(2 * span.start + c * half, LANES), half)
        for j in range(pair // LANES):
            part = slice(j * LANES, (j + 1) * LANES)
            merged = held[part, span].astype(F32) + mix_rate * rank_dot(joined[:, part], highs[:, cols])
            own_out[:, part] = merged.T.astype(BF16)
        keep_own(own_out, out.at[
            pl.ds(pl.multiple_of(c * half, 16), half), pl.ds(pl.multiple_of(pair * chip, LANES), pair)
        ])

    theirs = pl.ds(pl.multiple_of(rows * (1 - c), 16), rows)
    arrived(lows.at[:, 0], fetched.at[LOWS])
    arrived(highs, fetched.at[HIGHS])
    arrived(held.at[mine, :], fetched.at[TRAINS])
    arrived(lows.at[:, 0], swap_recv.at[1])
    arrived(held.at[theirs, :], swap_recv.at[0])
    merge(0, oq, own_q)
    for j in (2, 3):
        move(j, TO_X).start()
        move(n + j, TO_Y).start()
    merge(1, ok, own_k)
    merge(2, ov, own_v)
    for j in range(4, n):
        move(j, TO_X).start()
        move(n + j, TO_Y).start()
    small[0].wait()
    small.append(remote(both_rows, both_rows, nsend.at[1], nrecv.at[1], zero=at.yn))
    small[1].start()
    for j in range(n):
        move(n + j, TO_X).start()
        if j > 0:
            move(j, TO_Y).start()
    for k in range(2 * n):
        move(k, P_OWN).start()

    for j in range(n):
        come(j, 0)
        if j < EARLY:
            @pl.when(c == 1)
            def _():
                move(j, ON).start()
                move(n + j, ON).start()
        move(j, P_X).start()
        move(n + j, P_Y).start()
    small[1].wait()
    small.append(remote(on.at[c], on.at[c], nsend.at[2], nrecv.at[2], zero=at.partner))
    small[2].start()
    arrived(lows.at[:, 0], swap_send.at[1])
    arrived(held.at[mine, :], swap_send.at[0])
    arrived(share, keep)
    small[2].wait()
    for j in range(n):
        come(j, 1)
        move(n + j, P_X).start()
        move(j, P_Y).start()
    for kind in range(5):
        arrived(share, send.at[kind])
    for kind in range(3):
        arrived(share, across.at[kind])

    @pl.when(c == 1)
    def _():
        early = oq.at[: early_rows(units, rows, EARLY), :]
        arrived(early, early_send)
        arrived(early, early_recv)


def early_rows(units, rows, count):
    return 2 * sum(size * rows if a == 3 else size * 2 * rows for a, _, size in units[:count]) // (8 * rows)


def finish(zeros, widths, *refs):
    (
        _, oq, ok, ov, om, on, dq, dk, dv, dm, norm, every, flat,
        ready, copied, on_send, on_recv, send, recv, nsend, nrecv, psend, precv,
    ) = refs
    at = Place()
    c = at.c
    outs, diag = (oq, ok, ov, om), (dq, dk, dv, dm)
    rows = dm.shape[0] // 2
    mix, nq, nk = om.shape[1], oq.shape[0] // 2, ok.shape[0] // 2
    units = unit_list(rows, mix, nq, nk)
    n = len(units) // 2
    share = om.at[: rows * (mix + 2 * nq + 4 * nk) // mix, :]

    barrier = pltpu.get_barrier_semaphore()
    for other in (at.xn, at.yn):
        tell(barrier, zero=other)

    @pl.when(c == 0)
    def _():
        tell(barrier, zero=at.partner)

    @pl.when(c == 1)
    def _():
        for d in range(1, widths):
            tell(barrier, width=lax.rem(at.w + d, widths))

    pl.semaphore_wait(barrier, 2 + widths * c)
    pl.when(c == 1)(lambda: tell(ready, zero=at.partner))

    def onward(k):
        p, where = (at.chip_x, at.yn) if k < n else (at.chip_y, at.xn)
        return remote(
            region(units[k], outs, rows, p, c), region(units[k], diag, rows, 0, c), on_send, on_recv.at[k % n], zero=where
        )

    def across(k, early):
        there = region(units[k], diag, rows, 0, c)
        source = region(units[k], outs, rows, at.chip_d, c) if early else there
        return remote(source, there, send, recv, zero=at.partner)

    for j in range(n):
        for k in (j, n + j):
            if j < EARLY:
                pl.when(c == 0)(lambda k=k: onward(k).start())
            else:
                onward(k).start()

    others = every.at[: widths - 1]
    to_partner = remote(every, every, psend, precv, zero=at.partner)

    @pl.when(c == 1)
    def _():
        for d in range(1, widths):
            remote(on, every.at[at.w], nsend, nrecv, width=lax.rem(at.w + d, widths)).start()
        for j in range(EARLY):
            for k in (j, n + j):
                across(k, True).start()
                pltpu.make_async_copy(
                    region(units[k], outs, rows, at.chip_d, c), region(units[k], diag, rows, 0, c), copied
                ).start()
        every[at.w] = on[...]
        arrived(others, nsend)
        arrived(others, nrecv)
        to_partner.start()

    pl.when(c == 0)(lambda: pl.semaphore_wait(ready, 1))
    size = norm.shape[0] // (zeros * widths)
    for j in range(n):
        if j == n - 3:
            pl.when(c == 0)(lambda: to_partner.wait_recv())
            for zero in range(zeros):
                for w in range(widths):
                    i = zero * widths + w
                    flat[:, i * size : (i + 1) * size] = every[w, zero % 2, zero // 2][:, :size]
            norm[...] = flat[0, :].astype(BF16)

        def pass_on():
            a, _, size = units[j]
            arrived(dm.at[:rows, : 2 * size] if a == 3 else dq.at[: 2 * size, :], on_recv.at[j])
            across(j, False).start()
            across(n + j, False).start()

        if j < EARLY:
            pl.when(c == 0)(pass_on)
        else:
            pass_on()

    @pl.when(c == 0)
    def _():
        arrived(share, on_send)

    @pl.when(c == 1)
    def _():
        early = early_rows(units, rows, EARLY)
        if EARLY < n:
            arrived(oq.at[: early_rows(units, rows, n) - early, :], on_send)
        arrived(oq.at[:early, :], copied)
        to_partner.wait_send()

    arrived(share, send)
    arrived(share, recv)


def publish_most(rows, *refs):
    n = 4
    at = Place()
    token, done = refs[-2:]
    token[...] = jnp.zeros_like(token)
    pair = 2 * rows
    for p in (at.chip, at.chip_x, at.chip_y):
        for k, (src, dst) in enumerate(zip(refs[:n], refs[n : 2 * n])):
            block = pl.ds(pl.multiple_of(pair * p, LANES), pair)
            for e in range(2):
                if k == 3:
                    half = src.shape[1] // 2
                    where = (block, slice(e * half, (e + 1) * half))
                else:
                    half = src.shape[0] // 2
                    where = (slice(e * half, (e + 1) * half), block)
                pltpu.make_async_copy(src.at[where], dst.at[where], done.at[k]).start()
    for k, src in enumerate(refs[:n]):
        arrived(src.at[: 3 * pair, :] if k == 3 else src.at[:, : 3 * pair], done.at[k])


def publish_rest(rows, *refs):
    n = 4
    at = Place()
    sources, norm, outs, norm_out, done = refs[:n], refs[n], refs[2 * n + 1 : 3 * n + 1], refs[3 * n + 1], refs[-1]
    pair = 2 * rows
    block = pl.ds(pl.multiple_of(pair * at.chip_d, LANES), pair)
    for e in range(4):
        for k, (src, dst) in enumerate(zip(sources, outs)):
            if k in (1, 2) and e % 2:
                continue
            parts = 2 if k in (1, 2) else 4
            size = src.shape[1 if k == 3 else 0] // parts
            i = e * parts // 4
            if k == 3:
                at_i = slice(i * size, (i + 1) * size)
                pltpu.make_async_copy(src.at[:, at_i], dst.at[block, at_i], done.at[k]).start()
            else:
                at_i = slice(i * size, (i + 1) * size)
                pltpu.make_async_copy(src.at[at_i, :], dst.at[at_i, block], done.at[k]).start()
    pltpu.make_async_copy(norm, norm_out, done.at[n]).start()
    for k, src in enumerate((*sources, norm)):
        arrived(src, done.at[k])


def fast_body(zeros, widths, *args):
    tq, lq, hq, tk, lk, hk, tv, lv, hv, tm, lm, hm, nt, ns = args
    rows, depth = tq.shape[0], tq.shape[0] * zeros
    new = jax.ShapeDtypeStruct
    shapes = [(tq.shape[1], depth), (tk.shape[1], depth), (tv.shape[1], depth), (depth, tm.shape[0])]
    pair = 2 * rows
    held = 2 * sum(a * b for a, b in shapes)
    dma = pltpu.SemaphoreType.DMA
    count = len(unit_list(rows, tm.shape[0], tq.shape[1] // 2, tk.shape[1] // 2))
    moved = [tq, lq.T, hq, tk, lk.T, hk, tv, lv.T, hv, tm.T, lm.T, hm, nt[None, :], ns[None, :]]
    rank, mix = hm.shape[0], tm.shape[0]
    halves = (tq.shape[1] + tk.shape[1] + tv.shape[1]) // 2
    norms = (CORES, zeros // CORES, 1, LANES)
    in_vmem, in_hbm = pl.BlockSpec(memory_space=VMEM), pl.BlockSpec(memory_space=HBM)
    *most, on = pl.pallas_call(
        functools.partial(gather, zeros, widths),
        out_shape=[VMEM(s, BF16) for s in shapes] + [VMEM(norms, F32)],
        in_specs=[in_hbm] * len(args),
        out_specs=[in_vmem] * (len(shapes) + 1),
        scratch_shapes=[
            VMEM((rows, mix), BF16), VMEM((rank, mix + rows), BF16), VMEM((pair, halves), BF16),
            VMEM((3, 2, rank, rows), BF16), VMEM((rank, 2 * halves), BF16), VMEM((2, 1, nt.shape[0]), F32),
            VMEM((tq.shape[1] // 2, pair), BF16), VMEM((tk.shape[1] // 2, pair), BF16), VMEM((tv.shape[1] // 2, pair), BF16),
            VMEM((rows, mix), BF16), VMEM((rank, pair), BF16),
            dma((7,)), dma, dma((2,)), dma((2,)), dma((5,)), dma((count,)), dma((3,)), dma, dma, dma((3,)), dma((3,)),
        ],
        compiler_params=pltpu.CompilerParams(
            collective_id=0, has_side_effects=True, vmem_limit_bytes=VMEM_BYTES - held - 64 * 1024
        ),
        name="gather_merged",
    )(*moved)
    *done, token = pl.pallas_call(
        functools.partial(publish_most, rows),
        out_shape=[new(s, BF16) for s in shapes] + [VMEM((8, LANES), F32)],
        in_specs=[in_vmem] * len(shapes),
        out_specs=[in_hbm] * len(shapes) + [in_vmem],
        scratch_shapes=[dma((len(shapes),))],
        compiler_params=pltpu.CompilerParams(vmem_limit_bytes=2**20),
        name="publish_most",
    )(*most)
    part = [(s[0], pair) for s in shapes[:3]] + [(pair, shapes[3][1])]
    *rest, norm, _ = pl.pallas_call(
        functools.partial(finish, zeros, widths),
        out_shape=[VMEM(s, BF16) for s in part] + [VMEM((depth,), BF16), VMEM((widths, *norms), F32)],
        in_specs=[in_vmem] * (len(shapes) + 2),
        out_specs=[in_vmem] * (len(part) + 2),
        scratch_shapes=[
            VMEM((1, depth), F32), pltpu.SemaphoreType.REGULAR,
            dma, dma, dma((count // 2,)), dma, dma, dma, dma, dma, dma,
        ],
        compiler_params=pltpu.CompilerParams(collective_id=1, has_side_effects=True, vmem_limit_bytes=2**21),
        name="finish",
    )(token, *most, on)
    return pl.pallas_call(
        functools.partial(publish_rest, rows),
        out_shape=[new(s, BF16) for s in shapes] + [new((depth,), BF16)],
        in_specs=[in_vmem] * (len(shapes) + 1) + [in_hbm] * len(shapes),
        out_specs=[in_hbm] * (len(shapes) + 1),
        input_output_aliases={len(shapes) + 1 + k: k for k in range(len(shapes))},
        scratch_shapes=[dma((len(shapes) + 1,))],
        compiler_params=pltpu.CompilerParams(vmem_limit_bytes=2**20),
        name="publish_rest",
    )(*rest, norm, *done)


def solution(mesh):
    placed = (
        P("zero", "width"), P("zero", None), P(None, "width"),
        P("zero", "width"), P("zero", None), P(None, "width"),
        P("zero", "width"), P("zero", None), P(None, "width"),
        P("width", "zero"), P("width", None), P(None, "zero"),
        P(("zero", "width")), P(("zero", "width")),
    )
    zeros, widths = mesh.shape["zero"], mesh.shape["width"]
    side = math.isqrt(zeros // CORES)

    def body(*args):
        rows, nq, nk, mix = args[0].shape[0], args[0].shape[1] // 2, args[3].shape[1] // 2, args[9].shape[0]
        square = side == 2 and CORES * side * side == zeros and args[6].shape == args[3].shape
        even = (2 * nq + 4 * nk) % mix == 0 and rows % 64 == 0
        if square and even and nq % 128 == 0 and nk % 128 == 0 and mix % (4 * LANES) == 0:
            return fast_body(zeros, widths, *args)
        return plain_body(*args)

    return jax.shard_map(
        body,
        mesh=mesh,
        in_specs=placed,
        out_specs=(P("width", None), P("width", None), P("width", None), P(None, "width"), P()),
        check_vma=False,
    )
```

```python
import functools
import math

import jax
import jax.numpy as jnp
from jax import lax
from jax.experimental import pallas as pl
from jax.experimental.pallas import tpu as pltpu
from jax.sharding import PartitionSpec as P

mix_rate = 0.5
CORES = 2
LANES = 128
F32 = jnp.float32
BF16 = jnp.bfloat16
BOTH = 1
EARLY = 7
VMEM_BYTES = 67_043_328
VMEM = pltpu.VMEM
HBM = pltpu.MemorySpace.HBM
TO_X, TO_Y, ON, P_OWN, P_X, P_Y, P_D = range(7)


def plain_body(
    train_query, low_query, high_query, train_key, low_key, high_key, train_value, low_value, high_value,
    train_mixed, low_mixed, high_mixed, norm_train, norm_step,
):
    def merged(train, low, high):
        return (train.astype(F32) + mix_rate * jnp.dot(low, high, preferred_element_type=F32)).astype(BF16)

    return (
        lax.all_gather(merged(train_query, low_query, high_query), "zero", axis=0, tiled=True).T,
        lax.all_gather(merged(train_key, low_key, high_key), "zero", axis=0, tiled=True).T,
        lax.all_gather(merged(train_value, low_value, high_value), "zero", axis=0, tiled=True).T,
        lax.all_gather(merged(train_mixed, low_mixed, high_mixed).T, "zero", axis=0, tiled=True),
        lax.all_gather((norm_train + norm_step).astype(BF16), ("zero", "width"), axis=0, tiled=True),
    )


class Place:
    def __init__(self):
        self.me, self.w = lax.axis_index("zero"), lax.axis_index("width")
        me = self.me
        self.c = lax.rem(me, 2)
        x = lax.rem(lax.div(me, 2), 2)
        self.y = lax.div(me, 4)
        self.chip = lax.div(me, 2)
        self.partner, self.xn, self.yn = me + 1 - 2 * self.c, me + 2 - 4 * x, me + 4 - 8 * self.y
        self.chip_x, self.chip_y, self.chip_d = self.chip + 1 - 2 * x, self.chip + 2 - 4 * self.y, 3 - self.chip


def remote(src, dst, ssem, rsem, **where):
    return pltpu.make_async_remote_copy(
        src_ref=src, dst_ref=dst, send_sem=ssem, recv_sem=rsem, device_id=where, device_id_type=pl.DeviceIdType.MESH
    )


def tell(sem, **where):
    pl.semaphore_signal(sem, inc=1, device_id=where, device_id_type=pl.DeviceIdType.MESH)


def unit_list(rows, mix, nq, nk):
    eighth = mix // 8
    mixed = ((0, eighth), (eighth, eighth), (2 * eighth, 2 * eighth))
    query = ((0, nq // 4), (nq // 4, nq // 4))
    parts = ((0, nk // 2), (nk // 2, nk // 4), (3 * nk // 4, nk // 8), (7 * nk // 8, nk // 8))
    return [
        (a, at + half, size)
        for key, share in ((1, 0), (2, 1))
        for a, half, pieces in ((3, share * mix // 2, mixed), (0, share * nq // 2, query), (key, 0, parts))
        for at, size in pieces
    ]


def region(unit, outs, rows, chip, c):
    a, start, size = unit
    out = outs[a]
    if a == 3:
        return out.at[pl.ds(pl.multiple_of(rows * (2 * chip + c), 16), rows), start : start + size]
    pair = 2 * rows
    return out.at[
        pl.ds(pl.multiple_of(c * (out.shape[0] // 2) + start, 16), size), pl.ds(pl.multiple_of(pair * chip, LANES), pair)
    ]


def arrived(ref, sem):
    pltpu.make_async_copy(ref, ref, sem).wait()


def gather(
    zeros, widths,
    tq_h, lq_h, hq_h, tk_h, lk_h, hk_h, tv_h, lv_h, hv_h, tm_h, lm_h, hm_h, nt_h, ns_h,
    oq, ok, ov, om, on,
    tm, pair_m, held, lows, highs, gains, own_q, own_k, own_v, own_m, joined,
    fetched, keep, swap_send, swap_recv, send, arrive, across, on_send, on_recv, early_recv, nsend, nrecv,
):
    at = Place()
    c, chip = at.c, at.chip
    rows = tq_h.shape[0]
    pair = 2 * rows
    mix = tm_h.shape[1]
    outs = (oq, ok, ov, om)
    nq, nk = oq.shape[0] // 2, ok.shape[0] // 2
    units = unit_list(rows, mix, nq, nk)
    n = len(units) // 2
    first = units[0][2]
    share = om.at[: rows * (mix + 2 * nq + 4 * nk) // mix, :]
    LOW_HIGH, FIRST, OTHERS, GAINS, LOWS, HIGHS, TRAINS = range(7)

    def rank_dot(left, right):
        return lax.dot_general(left, right, (((0,), (0,)), ((), ())), preferred_element_type=F32)

    def fetch(src, dst, sem):
        pltpu.make_async_copy(src, dst, fetched.at[sem]).start()

    fetch(lm_h, pair_m.at[:, :mix], LOW_HIGH)
    fetch(hm_h, pair_m.at[:, mix:], LOW_HIGH)
    fetch(tm_h.at[:, :first], tm.at[:, :first], FIRST)
    barrier = pltpu.get_barrier_semaphore()
    for other in (at.partner, at.xn, at.yn):
        tell(barrier, zero=other)
    fetch(nt_h, gains.at[0], GAINS)
    fetch(ns_h, gains.at[1], GAINS)
    fetch(tm_h.at[:, first:], tm.at[:, first:], OTHERS)

    mine = pl.ds(pl.multiple_of(rows * c, 16), rows)
    spans, spot = [], 0
    for train in (tq_h, tk_h, tv_h):
        spans.append(slice(spot, spot + train.shape[1] // 2))
        spot += train.shape[1] // 2
    for k, (train, low, high) in enumerate(((tq_h, lq_h, hq_h), (tk_h, lk_h, hk_h), (tv_h, lv_h, hv_h))):
        half = train.shape[1] // 2
        cols = pl.ds(pl.multiple_of(c * half, LANES), half)
        fetch(train.at[:, cols], held.at[mine, spans[k]], TRAINS)
        fetch(low, lows.at[k, c], LOWS)
        fetch(high, highs.at[:, 2 * spans[k].start : 2 * spans[k].stop], HIGHS)

    def merge_mixed(start, size):
        cols = slice(start, start + size)
        merged = tm[:, cols].astype(F32) + mix_rate * rank_dot(pair_m[:, mix:], pair_m[:, cols])
        own_m[:, cols] = merged.astype(BF16)

    sources = [
        own_m.at[:, s : s + size] if a == 3 else (own_q, own_k, own_v)[a].at[s : s + size, :] for a, s, size in units
    ]

    def move(k, kind):
        p = {ON: at.chip_x if k < n else at.chip_y, P_X: at.chip_x, P_Y: at.chip_y, P_D: at.chip_d}.get(kind, chip)
        there = region(units[k], outs, rows, p, c)
        where = {TO_X: at.xn, TO_Y: at.yn, ON: at.yn if k < n else at.xn}.get(kind, at.partner)
        if kind in (TO_X, TO_Y):
            recv = arrive.at[k % n + (n if (kind == TO_X) == (k >= n) else 0)]
        elif kind == ON:
            recv = on_recv.at[k % n] if k % n < BOTH else early_recv
        else:
            recv = across.at[kind - P_OWN]
        return remote(
            sources[k] if kind in (TO_X, TO_Y, P_OWN) else there, there,
            on_send if kind == ON else send.at[kind - (kind > ON)], recv, zero=where,
        )

    def come(j, sem):
        a, _, size = units[j]
        arrived(om.at[:rows, : 2 * size] if a == 3 else oq.at[: 2 * size, :pair], sem)

    arrived(pair_m, fetched.at[LOW_HIGH])
    arrived(tm.at[:, :first], fetched.at[FIRST])
    merge_mixed(0, first)

    pl.semaphore_wait(barrier, 3)
    move(0, TO_X).start()
    move(0, TO_Y).start()
    for k, (train, low) in enumerate(((tq_h, lq_h), (tk_h, lk_h), (tv_h, lv_h))):
        half = train.shape[1] // 2
        cols = pl.ds(pl.multiple_of((1 - c) * half, LANES), half)
        remote(train.at[:, cols], held.at[mine, spans[k]], swap_send.at[0], swap_recv.at[0], zero=at.partner).start()
        remote(low, lows.at[k, c], swap_send.at[1], swap_recv.at[1], zero=at.partner).start()

    arrived(gains, fetched.at[GAINS])
    on[c, chip] = jnp.pad(gains[0] + gains[1], ((0, 0), (0, LANES - gains.shape[2])))
    arrived(tm.at[:, first:], fetched.at[OTHERS])
    for k in (n, 1, n + 1, 2, n + 2):
        merge_mixed(*units[k][1:])

    row = on.at[c, pl.ds(chip, 1)]
    both_rows = on.at[c, pl.ds(2 * at.y, 2)]
    small = [
        remote(row, row, nsend.at[0], nrecv.at[0], zero=at.xn),
        remote(both_rows, both_rows, nsend.at[1], nrecv.at[1], zero=at.yn),
        remote(on.at[c], on.at[c], nsend.at[2], nrecv.at[2], zero=at.partner),
    ]
    small[0].start()
    move(n, TO_Y).start()
    for j in (1, 2):
        move(j, TO_X).start()
        move(n + j, TO_Y).start()

    def keep_own(source, there):
        pltpu.make_async_copy(source, there, keep).start()

    keep_own(own_m, om.at[pl.ds(pl.multiple_of(rows * at.me, 16), rows), :])

    def merge(e, out, own_out):
        span = spans[e]
        half = span.stop - span.start
        joined[:, :rows] = lows[e, 0]
        joined[:, rows:] = lows[e, 1]
        cols = pl.ds(pl.multiple_of(2 * span.start + c * half, LANES), half)
        for j in range(pair // LANES):
            part = slice(j * LANES, (j + 1) * LANES)
            merged = held[part, span].astype(F32) + mix_rate * rank_dot(joined[:, part], highs[:, cols])
            own_out[:, part] = merged.T.astype(BF16)
        keep_own(own_out, out.at[
            pl.ds(pl.multiple_of(c * half, 16), half), pl.ds(pl.multiple_of(pair * chip, LANES), pair)
        ])

    theirs = pl.ds(pl.multiple_of(rows * (1 - c), 16), rows)
    arrived(lows.at[:, 0], fetched.at[LOWS])
    arrived(highs, fetched.at[HIGHS])
    arrived(held.at[mine, :], fetched.at[TRAINS])
    arrived(lows.at[:, 0], swap_recv.at[1])
    arrived(held.at[theirs, :], swap_recv.at[0])
    merge(0, oq, own_q)
    for j in (3, 4):
        move(j, TO_X).start()
        move(n + j, TO_Y).start()
    merge(1, ok, own_k)
    merge(2, ov, own_v)
    for j in range(5, n):
        move(j, TO_X).start()
        move(n + j, TO_Y).start()
    small[0].wait()
    small[1].start()
    for j in range(n):
        move(n + j, TO_X).start()
        if j > 0:
            move(j, TO_Y).start()
    for k in range(2 * n):
        move(k, P_OWN).start()

    def onward(j):
        move(j, ON).start()
        move(n + j, ON).start()

    for j in range(n):
        come(j, arrive.at[j])
        if j < BOTH:
            onward(j)
        elif j < EARLY:
            pl.when(c == 1)(lambda j=j: onward(j))
        move(j, P_X).start()
        move(n + j, P_Y).start()
    small[1].wait()
    small[2].start()
    arrived(lows.at[:, 0], swap_send.at[1])
    arrived(held.at[mine, :], swap_send.at[0])
    arrived(share, keep)
    small[2].wait()
    for j in range(n):
        come(j, arrive.at[n + j])
        move(n + j, P_X).start()
        move(j, P_Y).start()
    for j in range(BOTH):
        come(j, on_recv.at[j])
        move(j, P_D).start()
        move(n + j, P_D).start()
    for kind in range(5):
        arrived(share, send.at[kind])
    for kind in range(3):
        arrived(share, across.at[kind])
    common, early = early_rows(units, rows, BOTH), early_rows(units, rows, EARLY)
    if BOTH:
        arrived(oq.at[:common, :], send.at[5])
        arrived(oq.at[:common, :], across.at[3])
        pl.when(c == 0)(lambda: arrived(oq.at[:common, :], on_send))

    @pl.when(c == 1)
    def _():
        arrived(oq.at[:early, :], on_send)
        arrived(oq.at[: early - common, :], early_recv)


def early_rows(units, rows, count):
    return 2 * sum(size * rows if a == 3 else size * 2 * rows for a, _, size in units[:count]) // (8 * rows)


def finish(zeros, widths, *refs):
    (
        _, oq, ok, ov, om, on, dq, dk, dv, dm, norm,
        every, flat, ready, copied, on_send, on_recv, send, recv, nsend, nrecv,
    ) = refs
    at = Place()
    c = at.c
    outs, diag = (oq, ok, ov, om), (dq, dk, dv, dm)
    rows = dm.shape[0] // 2
    units = unit_list(rows, om.shape[1], oq.shape[0] // 2, ok.shape[0] // 2)
    n = len(units) // 2
    common, early, whole = (early_rows(units, rows, count) for count in (BOTH, EARLY, n))

    barrier = pltpu.get_barrier_semaphore()
    for other in (at.xn, at.yn):
        tell(barrier, zero=other)
    pl.when(c == 0)(lambda: tell(barrier, zero=at.partner))

    @pl.when(c == 1)
    def _():
        for d in range(1, widths):
            tell(barrier, width=lax.rem(at.w + d, widths))

    pl.semaphore_wait(barrier, 2 + widths * c)
    pl.when(c == 1)(lambda: tell(ready, zero=at.partner))

    def onward(j):
        for k in (j, n + j):
            p, where = (at.chip_x, at.yn) if k < n else (at.chip_y, at.xn)
            source, there = region(units[k], outs, rows, p, c), region(units[k], diag, rows, 0, c)
            remote(source, there, on_send, on_recv.at[j], zero=where).start()

    def across(j, early):
        for k in (j, n + j):
            there = region(units[k], diag, rows, 0, c)
            source = region(units[k], outs, rows, at.chip_d, c) if early else there
            remote(source, there, send, recv, zero=at.partner).start()
            if early:
                pltpu.make_async_copy(source, there, copied).start()

    for j in range(BOTH, n):
        if j < EARLY:
            pl.when(c == 0)(lambda j=j: onward(j))
        else:
            onward(j)

    to_partner = remote(every, every, nsend.at[0], nrecv.at[0], zero=at.partner)

    @pl.when(c == 1)
    def _():
        for d in range(1, widths):
            remote(on, every.at[at.w], nsend.at[1], nrecv.at[1], width=lax.rem(at.w + d, widths)).start()
        for j in range(BOTH, EARLY):
            across(j, True)
        every[at.w] = on[...]
        for sems in (nsend, nrecv):
            arrived(every.at[: widths - 1], sems.at[1])
        to_partner.start()

    pl.when(c == 0)(lambda: pl.semaphore_wait(ready, 1))
    size = norm.shape[0] // (zeros * widths)
    for j in range(BOTH, n):
        if j == n - 3:
            pl.when(c == 0)(lambda: to_partner.wait_recv())
            for zero in range(zeros):
                for w in range(widths):
                    i = zero * widths + w
                    flat[:, i * size : (i + 1) * size] = every[w, zero % 2, zero // 2][:, :size]
            norm[...] = flat[0, :].astype(BF16)

        def pass_on():
            a, _, size = units[j]
            arrived(dm.at[:rows, : 2 * size] if a == 3 else dq.at[: 2 * size, :], on_recv.at[j])
            across(j, False)

        if j < EARLY:
            pl.when(c == 0)(pass_on)
        else:
            pass_on()

    pl.when(c == 0)(lambda: arrived(oq.at[: whole - common, :], on_send))

    @pl.when(c == 1)
    def _():
        if EARLY < n:
            arrived(oq.at[: whole - early, :], on_send)
        arrived(oq.at[: early - common, :], copied)
        to_partner.wait_send()

    arrived(oq.at[: whole - common, :], send)
    arrived(oq.at[: whole - common, :], recv)


def publish_most(rows, *refs):
    n = 4
    at = Place()
    sources, outs, token, done = refs[:n], refs[n : 2 * n], *refs[2 * n :]
    token[...] = jnp.zeros_like(token)
    pair = 2 * rows
    for p in (at.chip, at.chip_x, at.chip_y):
        for k, (src, dst) in enumerate(zip(sources, outs)):
            block = pl.ds(pl.multiple_of(pair * p, LANES), pair)
            for e in range(2):
                if k == 3:
                    half = src.shape[1] // 2
                    where = (block, slice(e * half, (e + 1) * half))
                else:
                    half = src.shape[0] // 2
                    where = (slice(e * half, (e + 1) * half), block)
                pltpu.make_async_copy(src.at[where], dst.at[where], done.at[k]).start()
    oq, ok, _, om = sources
    units = unit_list(rows, om.shape[1], oq.shape[0] // 2, ok.shape[0] // 2)
    for k, unit in enumerate(units):
        if k % (len(units) // 2) < BOTH:
            for core in range(CORES):
                src, dst = (region(unit, arrays, rows, at.chip_d, core) for arrays in (sources, outs))
                pltpu.make_async_copy(src, dst, done.at[n]).start()
    for k, src in enumerate(sources):
        arrived(src.at[: 3 * pair, :] if k == 3 else src.at[:, : 3 * pair], done.at[k])
    if BOTH:
        arrived(oq.at[: 2 * early_rows(units, rows, BOTH), :], done.at[n])


def publish_rest(rows, *refs):
    n = 4
    at = Place()
    sources, norm, outs, norm_out, done = refs[:n], refs[n], refs[2 * n + 1 : 3 * n + 1], *refs[3 * n + 1 :]
    oq, ok, _, om = outs
    units = unit_list(rows, om.shape[1], oq.shape[0] // 2, ok.shape[0] // 2)
    half = len(units) // 2
    for j in range(BOTH, half):
        for k in (j, half + j):
            for core in range(CORES):
                src, dst = region(units[k], sources, rows, 0, core), region(units[k], outs, rows, at.chip_d, core)
                pltpu.make_async_copy(src, dst, done.at[0]).start()
    pltpu.make_async_copy(norm, norm_out, done.at[1]).start()
    arrived(oq.at[: 2 * (early_rows(units, rows, half) - early_rows(units, rows, BOTH)), :], done.at[0])
    arrived(norm, done.at[1])


def fast_body(zeros, widths, *args):
    tq, lq, hq, tk, lk, hk, tv, lv, hv, tm, lm, hm, nt, ns = args
    rows, depth = tq.shape[0], tq.shape[0] * zeros
    new = jax.ShapeDtypeStruct
    shapes = [(tq.shape[1], depth), (tk.shape[1], depth), (tv.shape[1], depth), (depth, tm.shape[0])]
    pair = 2 * rows
    held = 2 * sum(a * b for a, b in shapes)
    dma = pltpu.SemaphoreType.DMA
    count = len(unit_list(rows, tm.shape[0], tq.shape[1] // 2, tk.shape[1] // 2))
    moved = [tq, lq.T, hq, tk, lk.T, hk, tv, lv.T, hv, tm.T, lm.T, hm, nt[None, :], ns[None, :]]
    rank, mix = hm.shape[0], tm.shape[0]
    halves = (tq.shape[1] + tk.shape[1] + tv.shape[1]) // 2
    norms = (CORES, zeros // CORES, 1, LANES)
    in_vmem, in_hbm = pl.BlockSpec(memory_space=VMEM), pl.BlockSpec(memory_space=HBM)
    *most, on = pl.pallas_call(
        functools.partial(gather, zeros, widths),
        out_shape=[VMEM(s, BF16) for s in shapes] + [VMEM(norms, F32)],
        in_specs=[in_hbm] * len(args),
        out_specs=[in_vmem] * (len(shapes) + 1),
        scratch_shapes=[
            VMEM((rows, mix), BF16), VMEM((rank, mix + rows), BF16), VMEM((pair, halves), BF16),
            VMEM((3, 2, rank, rows), BF16), VMEM((rank, 2 * halves), BF16), VMEM((2, 1, nt.shape[0]), F32),
            VMEM((tq.shape[1] // 2, pair), BF16), VMEM((tk.shape[1] // 2, pair), BF16), VMEM((tv.shape[1] // 2, pair), BF16),
            VMEM((rows, mix), BF16), VMEM((rank, pair), BF16),
            dma((7,)), dma, dma((2,)), dma((2,)), dma((6,)), dma((count,)), dma((4,)),
            dma, dma((max(BOTH, 1),)), dma, dma((3,)), dma((3,)),
        ],
        compiler_params=pltpu.CompilerParams(
            collective_id=0, has_side_effects=True, vmem_limit_bytes=VMEM_BYTES - held - 64 * 1024
        ),
        name="gather_merged",
    )(*moved)
    *done, token = pl.pallas_call(
        functools.partial(publish_most, rows),
        out_shape=[new(s, BF16) for s in shapes] + [VMEM((8, LANES), F32)],
        in_specs=[in_vmem] * len(shapes),
        out_specs=[in_hbm] * len(shapes) + [in_vmem],
        scratch_shapes=[dma((len(shapes) + 1,))],
        compiler_params=pltpu.CompilerParams(vmem_limit_bytes=2**20),
        name="publish_most",
    )(*most)
    part = [(s[0], pair) for s in shapes[:3]] + [(pair, shapes[3][1])]
    *rest, norm = pl.pallas_call(
        functools.partial(finish, zeros, widths),
        out_shape=[VMEM(s, BF16) for s in part] + [VMEM((depth,), BF16)],
        in_specs=[in_vmem] * (len(shapes) + 2),
        out_specs=[in_vmem] * (len(part) + 1),
        scratch_shapes=[
            VMEM((widths, *norms), F32), VMEM((1, depth), F32),
            pltpu.SemaphoreType.REGULAR, dma, dma, dma((count // 2,)), dma, dma, dma((2,)), dma((2,)),
        ],
        compiler_params=pltpu.CompilerParams(collective_id=1, has_side_effects=True, vmem_limit_bytes=2**20),
        name="finish",
    )(token, *most, on)
    return pl.pallas_call(
        functools.partial(publish_rest, rows),
        out_shape=[new(s, BF16) for s in shapes] + [new((depth,), BF16)],
        in_specs=[in_vmem] * (len(shapes) + 1) + [in_hbm] * len(shapes),
        out_specs=[in_hbm] * (len(shapes) + 1),
        input_output_aliases={len(shapes) + 1 + k: k for k in range(len(shapes))},
        scratch_shapes=[dma((2,))],
        compiler_params=pltpu.CompilerParams(vmem_limit_bytes=2**20),
        name="publish_rest",
    )(*rest, norm, *done)


def solution(mesh):
    placed = (
        P("zero", "width"), P("zero", None), P(None, "width"),
        P("zero", "width"), P("zero", None), P(None, "width"),
        P("zero", "width"), P("zero", None), P(None, "width"),
        P("width", "zero"), P("width", None), P(None, "zero"),
        P(("zero", "width")), P(("zero", "width")),
    )
    zeros, widths = mesh.shape["zero"], mesh.shape["width"]
    side = math.isqrt(zeros // CORES)

    def body(*args):
        rows, nq, nk, mix = args[0].shape[0], args[0].shape[1] // 2, args[3].shape[1] // 2, args[9].shape[0]
        square = side == 2 and CORES * side * side == zeros and args[6].shape == args[3].shape
        even = (2 * nq + 4 * nk) % mix == 0 and rows % 64 == 0
        if square and even and nq % 128 == 0 and nk % 128 == 0 and mix % (8 * LANES) == 0:
            return fast_body(zeros, widths, *args)
        return plain_body(*args)

    return jax.shard_map(
        body,
        mesh=mesh,
        in_specs=placed,
        out_specs=(P("width", None), P("width", None), P("width", None), P(None, "width"), P()),
        check_vma=False,
    )
```

```python
import functools
import math

import jax
import jax.numpy as jnp
from jax import lax
from jax.experimental import pallas as pl
from jax.experimental.pallas import tpu as pltpu
from jax.sharding import PartitionSpec as P

mix_rate = 0.5
CORES = 2
LANES = 128
F32 = jnp.float32
BF16 = jnp.bfloat16
AHEAD = 8
BOTH = 3
EARLY = 9
TWICE = 1
VMEM_BYTES = 67_043_328
VMEM = pltpu.VMEM
HBM = pltpu.MemorySpace.HBM


def plain_body(
    train_query, low_query, high_query, train_key, low_key, high_key, train_value, low_value, high_value,
    train_mixed, low_mixed, high_mixed, norm_train, norm_step,
):
    def merged(train, low, high):
        return (train.astype(F32) + mix_rate * jnp.dot(low, high, preferred_element_type=F32)).astype(BF16)

    return (
        lax.all_gather(merged(train_query, low_query, high_query), "zero", axis=0, tiled=True).T,
        lax.all_gather(merged(train_key, low_key, high_key), "zero", axis=0, tiled=True).T,
        lax.all_gather(merged(train_value, low_value, high_value), "zero", axis=0, tiled=True).T,
        lax.all_gather(merged(train_mixed, low_mixed, high_mixed).T, "zero", axis=0, tiled=True),
        lax.all_gather((norm_train + norm_step).astype(BF16), ("zero", "width"), axis=0, tiled=True),
    )


class Place:
    def __init__(self):
        self.me, self.w = lax.axis_index("zero"), lax.axis_index("width")
        me = self.me
        self.c = lax.rem(me, 2)
        x = lax.rem(lax.div(me, 2), 2)
        self.y = lax.div(me, 4)
        self.chip = lax.div(me, 2)
        self.partner, self.xn, self.yn = me + 1 - 2 * self.c, me + 2 - 4 * x, me + 4 - 8 * self.y
        self.chip_x, self.chip_y, self.chip_d = self.chip + 1 - 2 * x, self.chip + 2 - 4 * self.y, 3 - self.chip


def remote(src, dst, ssem, rsem, **where):
    return pltpu.make_async_remote_copy(
        src_ref=src, dst_ref=dst, send_sem=ssem, recv_sem=rsem, device_id=where, device_id_type=pl.DeviceIdType.MESH
    )


def tell(sem, **where):
    pl.semaphore_signal(sem, inc=1, device_id=where, device_id_type=pl.DeviceIdType.MESH)


def unit_list(rows, mix, nq, nk):
    eighth = mix // 8
    mixed = ((0, eighth), (eighth, 2 * eighth), (3 * eighth, eighth))
    query = ((0, nq // 4), (nq // 4, nq // 4))
    parts = ((0, nk // 2), (nk // 2, nk // 4), (3 * nk // 4, nk // 8), (7 * nk // 8, nk // 8))
    return [
        (a, at + half, size)
        for key, share in ((1, 0), (2, 1))
        for a, half, pieces in ((3, share * mix // 2, mixed), (0, share * nq // 2, query), (key, 0, parts))
        for at, size in pieces
    ]


def region(unit, outs, rows, chip, c):
    a, start, size = unit
    out = outs[a]
    if a == 3:
        return out.at[pl.ds(pl.multiple_of(rows * (2 * chip + c), 16), rows), start : start + size]
    pair = 2 * rows
    return out.at[
        pl.ds(pl.multiple_of(c * (out.shape[0] // 2) + start, 16), size), pl.ds(pl.multiple_of(pair * chip, LANES), pair)
    ]


def arrived(ref, sem):
    pltpu.make_async_copy(ref, ref, sem).wait()


def gather(
    zeros, widths,
    tq_h, lq_h, hq_h, tk_h, lk_h, hk_h, tv_h, lv_h, hv_h, tm_h, lm_h, hm_h, nt_h, ns_h,
    oq, ok, ov, om, on,
    tm, pair_m, held, lows, highs, gains, own_q, own_k, own_v, own_m, joined,
    fetched, keep, swap_send, swap_recv, send, arrive, ahead_send, ahead_recv, cross_send, cross_recv, nsend, nrecv,
):
    at = Place()
    c, chip = at.c, at.chip
    rows = tq_h.shape[0]
    pair = 2 * rows
    mix = tm_h.shape[1]
    outs = (oq, ok, ov, om)
    nq, nk = oq.shape[0] // 2, ok.shape[0] // 2
    units = unit_list(rows, mix, nq, nk)
    n = len(units) // 2
    first = units[0][2]
    LOW_HIGH, FIRST, OTHERS, GAINS, LOWS, HIGHS, TRAINS = range(7)

    def rank_dot(left, right):
        return lax.dot_general(left, right, (((0,), (0,)), ((), ())), preferred_element_type=F32)

    def fetch(src, dst, sem):
        pltpu.make_async_copy(src, dst, fetched.at[sem]).start()

    fetch(lm_h, pair_m.at[:, :mix], LOW_HIGH)
    fetch(hm_h, pair_m.at[:, mix:], LOW_HIGH)
    fetch(tm_h.at[:, :first], tm.at[:, :first], FIRST)
    barrier = pltpu.get_barrier_semaphore()
    for other in (at.partner, at.xn, at.yn):
        tell(barrier, zero=other)
    fetch(nt_h, gains.at[0], GAINS)
    fetch(ns_h, gains.at[1], GAINS)
    fetch(tm_h.at[:, first:], tm.at[:, first:], OTHERS)

    mine = pl.ds(pl.multiple_of(rows * c, 16), rows)
    spans, spot = [], 0
    for train in (tq_h, tk_h, tv_h):
        spans.append(slice(spot, spot + train.shape[1] // 2))
        spot += train.shape[1] // 2
    for k, (train, low, high) in enumerate(((tq_h, lq_h, hq_h), (tk_h, lk_h, hk_h), (tv_h, lv_h, hv_h))):
        half = train.shape[1] // 2
        cols = pl.ds(pl.multiple_of(c * half, LANES), half)
        fetch(train.at[:, cols], held.at[mine, spans[k]], TRAINS)
        fetch(low, lows.at[k, c], LOWS)
        fetch(high, highs.at[:, 2 * spans[k].start : 2 * spans[k].stop], HIGHS)

    def merge_mixed(start, size):
        cols = slice(start, start + size)
        merged = tm[:, cols].astype(F32) + mix_rate * rank_dot(pair_m[:, mix:], pair_m[:, cols])
        own_m[:, cols] = merged.astype(BF16)

    sources = [
        own_m.at[:, s : s + size] if a == 3 else (own_q, own_k, own_v)[a].at[s : s + size, :] for a, s, size in units
    ]

    def link(k, along_x, ssem, rsem):
        there = region(units[k], outs, rows, chip, c)
        remote(sources[k], there, ssem, rsem, zero=at.xn if along_x else at.yn).start()

    def to_x(k):
        link(k, True, send, arrive.at[k])

    def to_y(k):
        link(k, False, send, arrive.at[k - n if k >= n else n])

    def cross(k, p):
        there = region(units[k], outs, rows, p, c)
        remote(sources[k] if p is chip else there, there, cross_send, cross_recv, zero=at.partner).start()

    arrived(pair_m, fetched.at[LOW_HIGH])
    arrived(tm.at[:, :first], fetched.at[FIRST])
    merge_mixed(0, first)

    pl.semaphore_wait(barrier, 3)
    to_x(0)
    to_y(0)
    for k, (train, low) in enumerate(((tq_h, lq_h), (tk_h, lk_h), (tv_h, lv_h))):
        half = train.shape[1] // 2
        cols = pl.ds(pl.multiple_of((1 - c) * half, LANES), half)
        remote(train.at[:, cols], held.at[mine, spans[k]], swap_send.at[0], swap_recv.at[0], zero=at.partner).start()
        remote(low, lows.at[k, c], swap_send.at[1], swap_recv.at[1], zero=at.partner).start()

    arrived(gains, fetched.at[GAINS])
    on[c, chip] = jnp.pad(gains[0] + gains[1], ((0, 0), (0, LANES - gains.shape[2])))
    arrived(tm.at[:, first:], fetched.at[OTHERS])
    for k in (n, 1, n + 1, 2, n + 2):
        merge_mixed(*units[k][1:])

    row = on.at[c, pl.ds(chip, 1)]
    both_rows = on.at[c, pl.ds(2 * at.y, 2)]
    small = [
        remote(row, row, nsend.at[0], nrecv.at[0], zero=at.xn),
        remote(both_rows, both_rows, nsend.at[1], nrecv.at[1], zero=at.yn),
        remote(on.at[c], on.at[c], nsend.at[2], nrecv.at[2], zero=at.partner),
    ]
    small[0].start()
    to_y(n)
    for j in (1, 2):
        to_x(j)
        to_y(n + j)

    def keep_own(source, there):
        pltpu.make_async_copy(source, there, keep).start()

    keep_own(own_m, om.at[pl.ds(pl.multiple_of(rows * at.me, 16), rows), :])

    def merge(e, out, own_out):
        span = spans[e]
        half = span.stop - span.start
        joined[:, :rows] = lows[e, 0]
        joined[:, rows:] = lows[e, 1]
        cols = pl.ds(pl.multiple_of(2 * span.start + c * half, LANES), half)
        for j in range(pair // LANES):
            part = slice(j * LANES, (j + 1) * LANES)
            merged = held[part, span].astype(F32) + mix_rate * rank_dot(joined[:, part], highs[:, cols])
            own_out[:, part] = merged.T.astype(BF16)
        keep_own(own_out, out.at[
            pl.ds(pl.multiple_of(c * half, 16), half), pl.ds(pl.multiple_of(pair * chip, LANES), pair)
        ])

    theirs = pl.ds(pl.multiple_of(rows * (1 - c), 16), rows)
    arrived(lows.at[:, 0], fetched.at[LOWS])
    arrived(highs, fetched.at[HIGHS])
    arrived(held.at[mine, :], fetched.at[TRAINS])
    arrived(lows.at[:, 0], swap_recv.at[1])
    arrived(held.at[theirs, :], swap_recv.at[0])
    merge(0, oq, own_q)
    small[0].wait()
    small[1].start()
    for j in (3, 4):
        to_x(j)
        to_y(n + j)
    merge(1, ok, own_k)
    merge(2, ov, own_v)
    for j in range(5, n):
        to_x(j)
        to_y(n + j)
    @pl.when(c == 1)
    def _():
        for j in range(AHEAD):
            for k in second_pair(j, n):
                link(k, k >= n, ahead_send, ahead_recv)

    for k in range(2 * n):
        cross(k, chip)
    lists = rows_of(units[:n])
    for j in range(n):
        arrived(oq.at[: rows_of([units[j]] * 2), :], arrive.at[j])
        cross(j, at.chip_x)
        cross(n + j, at.chip_y)
        if j == 0:
            arrived(oq.at[: rows_of(units[:1]), :], arrive.at[n])
            cross(0, at.chip_y)
        if j == n - 4:
            small[1].wait()
            small[2].start()
    arrived(lows.at[:, 0], swap_send.at[1])
    arrived(held.at[mine, :], swap_send.at[0])
    arrived(oq.at[: 2 * lists, :], keep)
    small[2].wait()
    phase = oq.at[: 2 * lists + rows_of(units[:1]), :]
    arrived(phase, send)
    arrived(oq.at[: 4 * lists + rows_of(units[:1]), :], cross_send)
    arrived(oq.at[: 4 * lists + rows_of(units[:1]), :], cross_recv)

    @pl.when(c == 1)
    def _():
        ahead = oq.at[: rows_of([units[k] for j in range(AHEAD) for k in second_pair(j, n)]), :]
        arrived(ahead, ahead_send)
        arrived(ahead, ahead_recv)


def second_pair(j, n):
    return (n + j, j) if j else (n,)


def rows_of(units):
    return sum(size // 8 if a == 3 else size // 4 for a, _, size in units)


def enter(at, z_peers, ready, told):
    c = at.c
    barrier = pltpu.get_barrier_semaphore()
    for other in (at.xn, at.yn):
        tell(barrier, zero=other)

    @pl.when(c == 1)
    def _():
        for w in z_peers:
            tell(barrier, width=w)

    pl.semaphore_wait(barrier, 2 + (1 + len(z_peers)) * c)
    pl.when(c == 0)(lambda: tell(barrier, zero=at.partner))

    @pl.when(c == 1)
    def _():
        for other in told:
            tell(ready, zero=other)


def spread(zeros, widths, *refs):
    (
        _, oq, ok, ov, om, on, xq, xk, xv, xm, yq, yk, yv, ym, dq, dk, dv, dm, norm,
        every, flat, ready, copied, send, arrive, on_send, on_recv, early_recv, cross_send, cross_recv, nsend, nrecv,
    ) = refs
    at = Place()
    c = at.c
    outs, from_x, from_y, diag = (oq, ok, ov, om), (xq, xk, xv, xm), (yq, yk, yv, ym), (dq, dk, dv, dm)
    rows = dm.shape[0] // 2
    units = unit_list(rows, om.shape[1], oq.shape[0] // 2, ok.shape[0] // 2)
    n = len(units) // 2
    z_peers = [lax.rem(at.w + d, widths) for d in range(1, widths)]
    enter(at, z_peers, ready, [at.partner])

    def own(j):
        for k in second_pair(j, n):
            source = region(units[k], outs, rows, at.chip, c)
            there = region(units[k], from_x if k >= n else from_y, rows, 0, c)
            remote(source, there, send, arrive.at[j], zero=at.xn if k >= n else at.yn).start()

    def onward(j):
        for k in (j, n + j):
            source = region(units[k], outs, rows, at.chip_x if k < n else at.chip_y, c)
            there = region(units[k], diag, rows, 0, c)
            recv = on_recv.at[j] if j < BOTH else early_recv
            remote(source, there, on_send, recv, zero=at.yn if k < n else at.xn).start()

    def across(j, ahead):
        for k in second_pair(j, n):
            there = region(units[k], from_x if k >= n else from_y, rows, 0, c)
            source = region(units[k], outs, rows, at.chip_x if k >= n else at.chip_y, c) if ahead else there
            remote(source, there, cross_send, cross_recv, zero=at.partner).start()
            if ahead:
                pltpu.make_async_copy(source, there, copied).start()

    def some(core_0_alone, step):
        pl.when(c == 0)(step) if core_0_alone else step()

    for j in range(n):
        some(j < AHEAD, lambda: own(j))
    for j in range(BOTH):
        onward(j)
    to_partner = remote(every, every, nsend.at[0], nrecv.at[0], zero=at.partner)

    @pl.when(c == 1)
    def _():
        for j in range(BOTH, EARLY):
            onward(j)
        for w in z_peers:
            remote(on, every.at[at.w], nsend.at[1], nrecv.at[1], width=w).start()
        for j in range(AHEAD):
            across(j, True)
        every[at.w] = on[...]
        for sems in (nsend, nrecv):
            arrived(every.at[: widths - 1], sems.at[1])
        to_partner.start()

    pl.when(c == 0)(lambda: pl.semaphore_wait(ready, 1))
    for j in range(n):

        def pass_on():
            arrived(oq.at[: rows_of([units[k] for k in second_pair(j, n)]), :], arrive.at[j])
            across(j, False)

        some(j < AHEAD, pass_on)
    size = norm.shape[0] // (zeros * widths)
    pl.when(c == 0)(lambda: to_partner.wait_recv())
    for zero in range(zeros):
        for w in range(widths):
            i = zero * widths + w
            flat[:, i * size : (i + 1) * size] = every[w, zero % 2, zero // 2][:, :size]
    norm[...] = flat[0, :].astype(BF16)
    for j in range(BOTH):
        arrived(oq.at[: 2 * rows_of(units[j : j + 1]), :], on_recv.at[j])
        for k in (j, n + j):
            there = region(units[k], diag, rows, 0, c)
            remote(there, there, cross_send, cross_recv, zero=at.partner).start()

    second = rows_of([units[k] for j in range(n) for k in second_pair(j, n)])
    ahead = rows_of([units[k] for j in range(AHEAD) for k in second_pair(j, n)])
    common, early = 2 * rows_of(units[:BOTH]), 2 * rows_of(units[:EARLY])

    @pl.when(c == 0)
    def _():
        arrived(oq.at[:second, :], send)
        arrived(oq.at[:common, :], on_send)

    arrived(oq.at[: second + common, :], cross_send)
    arrived(oq.at[: second + common, :], cross_recv)

    @pl.when(c == 1)
    def _():
        to_partner.wait_send()
        arrived(oq.at[:ahead, :], copied)
        if AHEAD < n:
            arrived(oq.at[: second - ahead, :], send)
        arrived(oq.at[:early, :], on_send)
        arrived(oq.at[: early - common, :], early_recv)


def finish(*refs):
    _, oq, ok, ov, om, dq, dk, dv, dm, rq, rk, rv, rm, ready, copied, on_send, on_recv, send, recv, last_recv = refs
    at = Place()
    c = at.c
    outs, held, diag = (oq, ok, ov, om), (dq, dk, dv, dm), (rq, rk, rv, rm)
    rows = rm.shape[0] // 2
    units = unit_list(rows, om.shape[1], oq.shape[0] // 2, ok.shape[0] // 2)
    n = len(units) // 2
    common, once, whole = (2 * rows_of(units[:count]) for count in (BOTH, n - TWICE, n))
    other_x, other_y = at.xn + at.partner - at.me, at.yn + at.partner - at.me
    enter(at, [], ready, [at.partner, other_x, other_y])

    def onward(j, other=False):
        for k in (j, n + j):
            source = region(units[k], outs, rows, at.chip_x if k < n else at.chip_y, c)
            there = region(units[k], diag, rows, 0, c)
            where = (other_y if k < n else other_x) if other else (at.yn if k < n else at.xn)
            remote(source, there, on_send, last_recv if other else on_recv.at[j], zero=where).start()

    def across(j, early):
        for k in (j, n + j):
            there = region(units[k], diag, rows, 0, c)
            source = region(units[k], held, rows, 0, c) if early else there
            remote(source, there, send, recv, zero=at.partner).start()
            if early:
                pltpu.make_async_copy(source, there, copied).start()

    @pl.when(c == 1)
    def _():
        for j in range(BOTH, n):
            across(j, True)
        arrived(oq.at[: whole - common, :], copied)
        arrived(oq.at[: whole - common, :], send)
        arrived(oq.at[: whole - once, :], last_recv)
        arrived(oq.at[: once - common, :], recv)

    @pl.when(c == 0)
    def _():
        for j in range(BOTH, n):
            onward(j)
        pl.semaphore_wait(ready, 3)
        for j in range(n - TWICE, n):
            onward(j, True)
        for j in range(BOTH, n):
            arrived(oq.at[: 2 * rows_of(units[j : j + 1]), :], on_recv.at[j])
            if j < n - TWICE:
                across(j, False)
        arrived(oq.at[: whole - common + whole - once, :], on_send)
        arrived(oq.at[: once - common, :], send)
        arrived(oq.at[: whole - common, :], recv)


def put_list(rows, sources, p, outs, q, key, second, skip, sem):
    pair = 2 * rows
    there = pl.ds(pl.multiple_of(pair * q, LANES), pair)
    here = there if p is q else pl.ds(pair * p, pair)
    om, oq = outs[3], outs[0]
    half, nq = om.shape[1] // 2, oq.shape[0] // 2
    places = [(3, slice(second * half + skip, (second + 1) * half)), (key, slice(None))]
    places += [(0, slice(c * nq + second * nq // 2, c * nq + (second + 1) * nq // 2)) for c in range(CORES)]
    for a, cut in places:
        src = sources[a].at[here, cut] if a == 3 else sources[a].at[cut, here]
        dst = outs[a].at[there, cut] if a == 3 else outs[a].at[cut, there]
        pltpu.make_async_copy(src, dst, sem).start()


def publish_first(rows, *refs):
    at = Place()
    sources, outs, (token, done) = refs[:4], refs[4:8], refs[8:]
    token[...] = jnp.zeros_like(token)
    pair = 2 * rows
    oq, ok, _, om = sources
    units = unit_list(rows, om.shape[1], oq.shape[0] // 2, ok.shape[0] // 2)
    first = units[0][2]
    for key, second in ((1, 0), (2, 1)):
        put_list(rows, sources, at.chip, outs, at.chip, key, second, 0, done.at[0])
    put_list(rows, sources, at.chip_x, outs, at.chip_x, 1, 0, 0, done.at[1])
    put_list(rows, sources, at.chip_y, outs, at.chip_y, 2, 1, 0, done.at[1])
    block = pl.ds(pl.multiple_of(pair * at.chip_y, LANES), pair)
    pltpu.make_async_copy(om.at[block, :first], outs[3].at[block, :first], done.at[1]).start()
    lists = rows_of(units[: len(units) // 2])
    arrived(oq.at[: 4 * lists, :], done.at[0])
    arrived(oq.at[: 4 * lists + 2 * rows_of(units[:1]), :], done.at[1])


def publish_next(rows, *refs):
    at = Place()
    from_x, from_y, diag, norm = refs[:4], refs[4:8], refs[8:12], refs[12]
    *outs, norm_out, token, done = refs[17:]
    token[...] = jnp.zeros_like(token)
    oq, ok, _, om = outs
    units = unit_list(rows, om.shape[1], oq.shape[0] // 2, ok.shape[0] // 2)
    n = len(units) // 2
    put_list(rows, from_x, 0, outs, at.chip_x, 2, 1, 0, done.at[0])
    put_list(rows, from_y, 0, outs, at.chip_y, 1, 0, units[0][2], done.at[0])
    for j in range(BOTH):
        put_pair(units, j, rows, diag, outs, at.chip_d, done.at[1])
    pltpu.make_async_copy(norm, norm_out, done.at[2]).start()
    arrived(oq.at[: 4 * rows_of(units[:n]) - 2 * rows_of(units[:1]), :], done.at[0])
    arrived(oq.at[: 4 * rows_of(units[:BOTH]), :], done.at[1])
    arrived(norm, done.at[2])


def put_pair(units, j, rows, sources, outs, q, sem):
    for k in (j, len(units) // 2 + j):
        for core in range(CORES):
            src, dst = region(units[k], sources, rows, 0, core), region(units[k], outs, rows, q, core)
            pltpu.make_async_copy(src, dst, sem).start()


def publish_last(rows, *refs):
    at = Place()
    sources, outs, done = refs[:4], refs[8:12], refs[12]
    oq, ok, _, om = outs
    units = unit_list(rows, om.shape[1], oq.shape[0] // 2, ok.shape[0] // 2)
    n = len(units) // 2
    for j in range(BOTH, n):
        put_pair(units, j, rows, sources, outs, at.chip_d, done)
    arrived(oq.at[: 4 * rows_of(units[BOTH:n]), :], done)


def fast_body(zeros, widths, *args):
    tq, lq, hq, tk, lk, hk, tv, lv, hv, tm, lm, hm, nt, ns = args
    rows, depth = tq.shape[0], tq.shape[0] * zeros
    new = jax.ShapeDtypeStruct
    shapes = [(tq.shape[1], depth), (tk.shape[1], depth), (tv.shape[1], depth), (depth, tm.shape[0])]
    pair = 2 * rows
    held = 2 * sum(a * b for a, b in shapes)
    dma = pltpu.SemaphoreType.DMA
    count = len(unit_list(rows, tm.shape[0], tq.shape[1] // 2, tk.shape[1] // 2))
    moved = [tq, lq.T, hq, tk, lk.T, hk, tv, lv.T, hv, tm.T, lm.T, hm, nt[None, :], ns[None, :]]
    rank, mix = hm.shape[0], tm.shape[0]
    halves = (tq.shape[1] + tk.shape[1] + tv.shape[1]) // 2
    norms = (CORES, zeros // CORES, 1, LANES)
    in_vmem, in_hbm = pl.BlockSpec(memory_space=VMEM), pl.BlockSpec(memory_space=HBM)
    *most, on = pl.pallas_call(
        functools.partial(gather, zeros, widths),
        out_shape=[VMEM(s, BF16) for s in shapes] + [VMEM(norms, F32)],
        in_specs=[in_hbm] * len(args),
        out_specs=[in_vmem] * (len(shapes) + 1),
        scratch_shapes=[
            VMEM((rows, mix), BF16), VMEM((rank, mix + rows), BF16), VMEM((pair, halves), BF16),
            VMEM((3, 2, rank, rows), BF16), VMEM((rank, 2 * halves), BF16), VMEM((2, 1, nt.shape[0]), F32),
            VMEM((tq.shape[1] // 2, pair), BF16), VMEM((tk.shape[1] // 2, pair), BF16), VMEM((tv.shape[1] // 2, pair), BF16),
            VMEM((rows, mix), BF16), VMEM((rank, pair), BF16),
            dma((7,)), dma, dma((2,)), dma((2,)), dma, dma((count // 2 + 1,)), dma, dma, dma, dma, dma((3,)), dma((3,)),
        ],
        compiler_params=pltpu.CompilerParams(
            collective_id=0, has_side_effects=True, vmem_limit_bytes=VMEM_BYTES - held - 64 * 1024
        ),
        name="gather_merged",
    )(*moved)
    results = [new(s, BF16) for s in shapes]
    token = VMEM((8, LANES), F32)
    *done, went = pl.pallas_call(
        functools.partial(publish_first, rows),
        out_shape=results + [token],
        in_specs=[in_vmem] * 4,
        out_specs=[in_hbm] * 4 + [in_vmem],
        scratch_shapes=[dma((2,))],
        compiler_params=pltpu.CompilerParams(vmem_limit_bytes=2**20),
        name="publish_first",
    )(*most)
    part = [VMEM((s[0], pair), BF16) for s in shapes[:3]] + [VMEM((pair, shapes[3][1]), BF16)]
    *more, norm = pl.pallas_call(
        functools.partial(spread, zeros, widths),
        out_shape=part * 3 + [VMEM((depth,), BF16)],
        in_specs=[in_vmem] * 6,
        out_specs=[in_vmem] * 13,
        scratch_shapes=[
            VMEM((widths, *norms), F32), VMEM((1, depth), F32),
            pltpu.SemaphoreType.REGULAR, dma, dma, dma((count // 2,)), dma, dma((BOTH,)), dma, dma, dma, dma((2,)), dma((2,)),
        ],
        compiler_params=pltpu.CompilerParams(collective_id=1, has_side_effects=True, vmem_limit_bytes=2**20),
        name="spread",
    )(went, *most, on)
    *done, gain, went = pl.pallas_call(
        functools.partial(publish_next, rows),
        out_shape=results + [new((depth,), BF16), token],
        in_specs=[in_vmem] * 13 + [in_hbm] * 4,
        out_specs=[in_hbm] * 5 + [in_vmem],
        input_output_aliases={13 + k: k for k in range(4)},
        scratch_shapes=[dma((3,))],
        compiler_params=pltpu.CompilerParams(vmem_limit_bytes=2**20),
        name="publish_next",
    )(*more, norm, *done)
    rest = pl.pallas_call(
        finish,
        out_shape=part,
        in_specs=[in_vmem] * 9,
        out_specs=[in_vmem] * 4,
        scratch_shapes=[pltpu.SemaphoreType.REGULAR, dma, dma, dma((count // 2,)), dma, dma, dma],
        compiler_params=pltpu.CompilerParams(collective_id=2, has_side_effects=True, vmem_limit_bytes=2**20),
        name="finish",
    )(went, *most, *more[8:])
    full = pl.pallas_call(
        functools.partial(publish_last, rows),
        out_shape=results,
        in_specs=[in_vmem] * 4 + [in_hbm] * 4,
        out_specs=[in_hbm] * 4,
        input_output_aliases={4 + k: k for k in range(4)},
        scratch_shapes=[dma],
        compiler_params=pltpu.CompilerParams(vmem_limit_bytes=2**20),
        name="publish_last",
    )(*rest, *done)
    return (*full, gain)


def solution(mesh):
    placed = (
        P("zero", "width"), P("zero", None), P(None, "width"),
        P("zero", "width"), P("zero", None), P(None, "width"),
        P("zero", "width"), P("zero", None), P(None, "width"),
        P("width", "zero"), P("width", None), P(None, "zero"),
        P(("zero", "width")), P(("zero", "width")),
    )
    zeros, widths = mesh.shape["zero"], mesh.shape["width"]
    side = math.isqrt(zeros // CORES)

    def body(*args):
        rows, nq, nk, mix = args[0].shape[0], args[0].shape[1] // 2, args[3].shape[1] // 2, args[9].shape[0]
        square = side == 2 and CORES * side * side == zeros and args[6].shape == args[3].shape
        even = (2 * nq + 4 * nk) % mix == 0 and rows % 64 == 0
        if square and even and nq % 128 == 0 and nk % 128 == 0 and mix % (8 * LANES) == 0:
            return fast_body(zeros, widths, *args)
        return plain_body(*args)

    return jax.shard_map(
        body,
        mesh=mesh,
        in_specs=placed,
        out_specs=(P("width", None), P("width", None), P("width", None), P(None, "width"), P()),
        check_vma=False,
    )
```

```python
import functools
import math

import jax
import jax.numpy as jnp
from jax import lax
from jax.experimental import pallas as pl
from jax.experimental.pallas import tpu as pltpu
from jax.sharding import PartitionSpec as P

mix_rate = 0.5
CORES = 2
LANES = 128
F32 = jnp.float32
BF16 = jnp.bfloat16
AHEAD = 8
BOTH = 4
EARLY = 9
TWICE = 1
VMEM_BYTES = 67_043_328
VMEM = pltpu.VMEM
HBM = pltpu.MemorySpace.HBM


def plain_body(
    train_query, low_query, high_query, train_key, low_key, high_key, train_value, low_value, high_value,
    train_mixed, low_mixed, high_mixed, norm_train, norm_step,
):
    def merged(train, low, high):
        return (train.astype(F32) + mix_rate * jnp.dot(low, high, preferred_element_type=F32)).astype(BF16)

    return (
        lax.all_gather(merged(train_query, low_query, high_query), "zero", axis=0, tiled=True).T,
        lax.all_gather(merged(train_key, low_key, high_key), "zero", axis=0, tiled=True).T,
        lax.all_gather(merged(train_value, low_value, high_value), "zero", axis=0, tiled=True).T,
        lax.all_gather(merged(train_mixed, low_mixed, high_mixed).T, "zero", axis=0, tiled=True),
        lax.all_gather((norm_train + norm_step).astype(BF16), ("zero", "width"), axis=0, tiled=True),
    )


class Place:
    def __init__(self):
        self.me, self.w = lax.axis_index("zero"), lax.axis_index("width")
        me = self.me
        self.c = lax.rem(me, 2)
        x = lax.rem(lax.div(me, 2), 2)
        self.y = lax.div(me, 4)
        self.chip = lax.div(me, 2)
        self.partner, self.xn, self.yn = me + 1 - 2 * self.c, me + 2 - 4 * x, me + 4 - 8 * self.y
        self.chip_x, self.chip_y, self.chip_d = self.chip + 1 - 2 * x, self.chip + 2 - 4 * self.y, 3 - self.chip


def remote(src, dst, ssem, rsem, **where):
    return pltpu.make_async_remote_copy(
        src_ref=src, dst_ref=dst, send_sem=ssem, recv_sem=rsem, device_id=where, device_id_type=pl.DeviceIdType.MESH
    )


def tell(sem, **where):
    pl.semaphore_signal(sem, inc=1, device_id=where, device_id_type=pl.DeviceIdType.MESH)


def unit_list(rows, mix, nq, nk):
    eighth = mix // 8
    mixed = ((0, eighth), (eighth, 2 * eighth), (3 * eighth, eighth))
    query = ((0, nq // 8), (nq // 8, 3 * nq // 8))
    parts = ((0, nk // 2), (nk // 2, nk // 4), (3 * nk // 4, nk // 8), (7 * nk // 8, nk // 8))
    return [
        (a, at + half, size)
        for key, share in ((1, 0), (2, 1))
        for a, half, pieces in ((3, share * mix // 2, mixed), (0, share * nq // 2, query), (key, 0, parts))
        for at, size in pieces
    ]


def region(unit, outs, rows, chip, c):
    a, start, size = unit
    out = outs[a]
    if a == 3:
        return out.at[pl.ds(pl.multiple_of(rows * (2 * chip + c), 16), rows), start : start + size]
    pair = 2 * rows
    return out.at[
        pl.ds(pl.multiple_of(c * (out.shape[0] // 2) + start, 16), size), pl.ds(pl.multiple_of(pair * chip, LANES), pair)
    ]


def arrived(ref, sem):
    pltpu.make_async_copy(ref, ref, sem).wait()


def gather(
    zeros, widths,
    tq_h, lq_h, hq_h, tk_h, lk_h, hk_h, tv_h, lv_h, hv_h, tm_h, lm_h, hm_h, nt_h, ns_h,
    oq, ok, ov, om, on,
    tm, pair_m, held, lows, highs, gains, own_q, own_k, own_v, own_m, joined,
    fetched, keep, swap_send, swap_recv, send, arrive, ahead_send, ahead_recv, cross_send, cross_recv, nsend, nrecv,
):
    at = Place()
    c, chip = at.c, at.chip
    rows = tq_h.shape[0]
    pair = 2 * rows
    mix = tm_h.shape[1]
    outs = (oq, ok, ov, om)
    nq, nk = oq.shape[0] // 2, ok.shape[0] // 2
    units = unit_list(rows, mix, nq, nk)
    n = len(units) // 2
    first = units[0][2]
    LOW_HIGH, FIRST, OTHERS, GAINS, LOWS, HIGHS, TRAINS = range(7)

    def rank_dot(left, right):
        return lax.dot_general(left, right, (((0,), (0,)), ((), ())), preferred_element_type=F32)

    def fetch(src, dst, sem):
        pltpu.make_async_copy(src, dst, fetched.at[sem]).start()

    barrier = pltpu.get_barrier_semaphore()
    for other in (at.xn, at.yn, at.partner):
        tell(barrier, zero=other)

    fetch(tm_h.at[:, :first], tm.at[:, :first], FIRST)
    fetch(hm_h, pair_m.at[:, mix:], LOW_HIGH)
    fetch(lm_h, pair_m.at[:, :mix], LOW_HIGH)
    fetch(nt_h, gains.at[0], GAINS)
    fetch(ns_h, gains.at[1], GAINS)
    fetch(tm_h.at[:, first:], tm.at[:, first:], OTHERS)

    mine = pl.ds(pl.multiple_of(rows * c, 16), rows)
    spans, spot = [], 0
    for train in (tq_h, tk_h, tv_h):
        spans.append(slice(spot, spot + train.shape[1] // 2))
        spot += train.shape[1] // 2
    for k, (train, low, high) in enumerate(((tq_h, lq_h, hq_h), (tk_h, lk_h, hk_h), (tv_h, lv_h, hv_h))):
        half = train.shape[1] // 2
        cols = pl.ds(pl.multiple_of(c * half, LANES), half)
        fetch(train.at[:, cols], held.at[mine, spans[k]], TRAINS)
        fetch(low, lows.at[k, c], LOWS)
        fetch(high, highs.at[:, 2 * spans[k].start : 2 * spans[k].stop], HIGHS)

    def merge_mixed(start, size):
        cols = slice(start, start + size)
        merged = tm[:, cols].astype(F32) + mix_rate * rank_dot(pair_m[:, mix:], pair_m[:, cols])
        own_m[:, cols] = merged.astype(BF16)

    sources = [
        own_m.at[:, s : s + size] if a == 3 else (own_q, own_k, own_v)[a].at[s : s + size, :] for a, s, size in units
    ]

    def link(k, along_x, ssem, rsem):
        there = region(units[k], outs, rows, chip, c)
        remote(sources[k], there, ssem, rsem, zero=at.xn if along_x else at.yn).start()

    def to_x(k):
        link(k, True, send, arrive.at[k])

    def to_y(k):
        link(k, False, send, arrive.at[k - n if k >= n else n])

    def cross(k, p):
        there = region(units[k], outs, rows, p, c)
        remote(sources[k] if p is chip else there, there, cross_send, cross_recv, zero=at.partner).start()

    arrived(pair_m, fetched.at[LOW_HIGH])
    arrived(tm.at[:, :first], fetched.at[FIRST])
    merge_mixed(0, first)

    pl.semaphore_wait(barrier, 3)
    to_x(0)
    to_y(0)
    for k, (train, low) in enumerate(((tq_h, lq_h), (tk_h, lk_h), (tv_h, lv_h))):
        half = train.shape[1] // 2
        cols = pl.ds(pl.multiple_of((1 - c) * half, LANES), half)
        remote(train.at[:, cols], held.at[mine, spans[k]], swap_send.at[0], swap_recv.at[0], zero=at.partner).start()
        remote(low, lows.at[k, c], swap_send.at[1], swap_recv.at[1], zero=at.partner).start()

    arrived(gains, fetched.at[GAINS])
    on[c, chip] = jnp.pad(gains[0] + gains[1], ((0, 0), (0, LANES - gains.shape[2])))
    arrived(tm.at[:, first:], fetched.at[OTHERS])
    for k in (n, 1, n + 1, 2, n + 2):
        merge_mixed(*units[k][1:])

    row = on.at[c, pl.ds(chip, 1)]
    both_rows = on.at[c, pl.ds(2 * at.y, 2)]
    small = [
        remote(row, row, nsend.at[0], nrecv.at[0], zero=at.xn),
        remote(both_rows, both_rows, nsend.at[1], nrecv.at[1], zero=at.yn),
        remote(on.at[c], on.at[c], nsend.at[2], nrecv.at[2], zero=at.partner),
    ]
    small[0].start()
    to_y(n)
    for j in (1, 2):
        to_x(j)
        to_y(n + j)

    def keep_own(source, there):
        pltpu.make_async_copy(source, there, keep).start()

    keep_own(own_m, om.at[pl.ds(pl.multiple_of(rows * at.me, 16), rows), :])

    def merge(e, out, own_out):
        span = spans[e]
        half = span.stop - span.start
        joined[:, :rows] = lows[e, 0]
        joined[:, rows:] = lows[e, 1]
        cols = pl.ds(pl.multiple_of(2 * span.start + c * half, LANES), half)
        for j in range(pair // LANES):
            part = slice(j * LANES, (j + 1) * LANES)
            merged = held[part, span].astype(F32) + mix_rate * rank_dot(joined[:, part], highs[:, cols])
            own_out[:, part] = merged.T.astype(BF16)
        keep_own(own_out, out.at[
            pl.ds(pl.multiple_of(c * half, 16), half), pl.ds(pl.multiple_of(pair * chip, LANES), pair)
        ])

    theirs = pl.ds(pl.multiple_of(rows * (1 - c), 16), rows)
    arrived(lows.at[:, 0], fetched.at[LOWS])
    arrived(highs, fetched.at[HIGHS])
    arrived(held.at[mine, :], fetched.at[TRAINS])
    arrived(lows.at[:, 0], swap_recv.at[1])
    arrived(held.at[theirs, :], swap_recv.at[0])
    merge(0, oq, own_q)
    small[0].wait()
    small[1].start()
    for j in (3, 4):
        to_x(j)
        to_y(n + j)
    merge(1, ok, own_k)
    merge(2, ov, own_v)
    for j in range(5, n):
        to_x(j)
        to_y(n + j)
    @pl.when(c == 1)
    def _():
        for j in range(AHEAD):
            for k in second_pair(j, n):
                link(k, k >= n, ahead_send, ahead_recv)

    for k in range(2 * n):
        cross(k, chip)
    lists = rows_of(units[:n])
    for j in range(n):
        arrived(oq.at[: rows_of([units[j]] * 2), :], arrive.at[j])
        cross(j, at.chip_x)
        cross(n + j, at.chip_y)
        if j == 0:
            arrived(oq.at[: rows_of(units[:1]), :], arrive.at[n])
            cross(0, at.chip_y)
        if j == n - 4:
            small[1].wait()
            small[2].start()
    arrived(lows.at[:, 0], swap_send.at[1])
    arrived(held.at[mine, :], swap_send.at[0])
    arrived(oq.at[: 2 * lists, :], keep)
    small[2].wait()
    phase = oq.at[: 2 * lists + rows_of(units[:1]), :]
    arrived(phase, send)
    arrived(oq.at[: 4 * lists + rows_of(units[:1]), :], cross_send)
    arrived(oq.at[: 4 * lists + rows_of(units[:1]), :], cross_recv)

    @pl.when(c == 1)
    def _():
        ahead = oq.at[: rows_of([units[k] for j in range(AHEAD) for k in second_pair(j, n)]), :]
        arrived(ahead, ahead_send)
        arrived(ahead, ahead_recv)


def second_pair(j, n):
    return (n + j, j) if j else (n,)


def rows_of(units):
    return sum(size // 8 if a == 3 else size // 4 for a, _, size in units)


def enter(at, z_peers, ready, told):
    c = at.c
    barrier = pltpu.get_barrier_semaphore()
    for other in (at.xn, at.yn):
        tell(barrier, zero=other)

    @pl.when(c == 1)
    def _():
        for w in z_peers:
            tell(barrier, width=w)

    pl.semaphore_wait(barrier, 2 + (1 + len(z_peers)) * c)
    pl.when(c == 0)(lambda: tell(barrier, zero=at.partner))

    @pl.when(c == 1)
    def _():
        for other in told:
            tell(ready, zero=other)


def spread(zeros, widths, *refs):
    (
        _, oq, ok, ov, om, on, xq, xk, xv, xm, yq, yk, yv, ym, dq, dk, dv, dm, norm,
        every, flat, ready, copied, send, arrive, on_send, on_recv, early_recv, cross_send, cross_recv, nsend, nrecv,
    ) = refs
    at = Place()
    c = at.c
    outs, from_x, from_y, diag = (oq, ok, ov, om), (xq, xk, xv, xm), (yq, yk, yv, ym), (dq, dk, dv, dm)
    rows = dm.shape[0] // 2
    units = unit_list(rows, om.shape[1], oq.shape[0] // 2, ok.shape[0] // 2)
    n = len(units) // 2
    z_peers = [lax.rem(at.w + d, widths) for d in range(1, widths)]
    enter(at, z_peers, ready, [at.partner])

    def own(j):
        for k in second_pair(j, n):
            source = region(units[k], outs, rows, at.chip, c)
            there = region(units[k], from_x if k >= n else from_y, rows, 0, c)
            remote(source, there, send, arrive.at[j], zero=at.xn if k >= n else at.yn).start()

    def onward(j):
        for k in (j, n + j):
            source = region(units[k], outs, rows, at.chip_x if k < n else at.chip_y, c)
            there = region(units[k], diag, rows, 0, c)
            recv = on_recv.at[j] if j < BOTH else early_recv
            remote(source, there, on_send, recv, zero=at.yn if k < n else at.xn).start()

    def across(j, ahead):
        for k in second_pair(j, n):
            there = region(units[k], from_x if k >= n else from_y, rows, 0, c)
            source = region(units[k], outs, rows, at.chip_x if k >= n else at.chip_y, c) if ahead else there
            remote(source, there, cross_send, cross_recv, zero=at.partner).start()
            if ahead:
                pltpu.make_async_copy(source, there, copied).start()

    def some(core_0_alone, step):
        pl.when(c == 0)(step) if core_0_alone else step()

    def send_all(first, pairs):
        for j in range(first, n):
            own(j)
        for j in range(pairs):
            onward(j)

    pl.when(c == 0)(lambda: send_all(0, BOTH))
    to_partner = remote(every, every, nsend.at[0], nrecv.at[0], zero=at.partner)

    @pl.when(c == 1)
    def _():
        for w in z_peers:
            remote(on, every.at[at.w], nsend.at[1], nrecv.at[1], width=w).start()
        for j in range(AHEAD):
            across(j, True)
        every[at.w] = on[...]
        for sems in (nsend, nrecv):
            arrived(every.at[: widths - 1], sems.at[1])
        send_all(AHEAD, EARLY)
        to_partner.start()

    pl.when(c == 0)(lambda: pl.semaphore_wait(ready, 1))
    for j in range(n):

        def pass_on():
            arrived(oq.at[: rows_of([units[k] for k in second_pair(j, n)]), :], arrive.at[j])
            across(j, False)

        some(j < AHEAD, pass_on)
    size = norm.shape[0] // (zeros * widths)
    pl.when(c == 0)(lambda: to_partner.wait_recv())
    for zero in range(zeros):
        for w in range(widths):
            i = zero * widths + w
            flat[:, i * size : (i + 1) * size] = every[w, zero % 2, zero // 2][:, :size]
    norm[...] = flat[0, :].astype(BF16)
    for j in range(BOTH):
        arrived(oq.at[: 2 * rows_of(units[j : j + 1]), :], on_recv.at[j])
        for k in (j, n + j):
            there = region(units[k], diag, rows, 0, c)
            remote(there, there, cross_send, cross_recv, zero=at.partner).start()

    second = rows_of([units[k] for j in range(n) for k in second_pair(j, n)])
    ahead = rows_of([units[k] for j in range(AHEAD) for k in second_pair(j, n)])
    common, early = 2 * rows_of(units[:BOTH]), 2 * rows_of(units[:EARLY])

    @pl.when(c == 0)
    def _():
        arrived(oq.at[:second, :], send)
        arrived(oq.at[:common, :], on_send)

    arrived(oq.at[: second + common, :], cross_send)
    arrived(oq.at[: second + common, :], cross_recv)

    @pl.when(c == 1)
    def _():
        to_partner.wait_send()
        arrived(oq.at[:ahead, :], copied)
        if AHEAD < n:
            arrived(oq.at[: second - ahead, :], send)
        arrived(oq.at[:early, :], on_send)
        arrived(oq.at[: early - common, :], early_recv)


def finish(*refs):
    _, oq, ok, ov, om, dq, dk, dv, dm, rq, rk, rv, rm, ready, copied, on_send, on_recv, send, recv, last_recv = refs
    at = Place()
    c = at.c
    outs, held, diag = (oq, ok, ov, om), (dq, dk, dv, dm), (rq, rk, rv, rm)
    rows = rm.shape[0] // 2
    units = unit_list(rows, om.shape[1], oq.shape[0] // 2, ok.shape[0] // 2)
    n = len(units) // 2
    common, once, whole = (2 * rows_of(units[:count]) for count in (BOTH, n - TWICE, n))
    other_x, other_y = at.xn + at.partner - at.me, at.yn + at.partner - at.me
    enter(at, [], ready, [at.partner, other_x, other_y])

    def onward(j, other=False):
        for k in (j, n + j):
            source = region(units[k], outs, rows, at.chip_x if k < n else at.chip_y, c)
            there = region(units[k], diag, rows, 0, c)
            where = (other_y if k < n else other_x) if other else (at.yn if k < n else at.xn)
            remote(source, there, on_send, last_recv if other else on_recv.at[j - BOTH], zero=where).start()

    def across(j, early):
        for k in (j, n + j):
            there = region(units[k], diag, rows, 0, c)
            source = region(units[k], held, rows, 0, c) if early else there
            remote(source, there, send, recv, zero=at.partner).start()
            if early:
                pltpu.make_async_copy(source, there, copied).start()

    @pl.when(c == 1)
    def _():
        for j in range(BOTH, n):
            across(j, True)
        arrived(oq.at[: whole - common, :], copied)
        arrived(oq.at[: whole - common, :], send)
        arrived(oq.at[: whole - once, :], last_recv)
        arrived(oq.at[: once - common, :], recv)

    @pl.when(c == 0)
    def _():
        for j in range(BOTH, n):
            onward(j)
        pl.semaphore_wait(ready, 3)
        for j in range(n - TWICE, n):
            onward(j, True)
        for j in range(BOTH, n):
            arrived(oq.at[: 2 * rows_of(units[j : j + 1]), :], on_recv.at[j - BOTH])
            if j < n - TWICE:
                across(j, False)
        arrived(oq.at[: whole - common + whole - once, :], on_send)
        arrived(oq.at[: once - common, :], send)
        arrived(oq.at[: whole - common, :], recv)


def put_list(rows, sources, p, outs, q, key, second, skip, sem):
    pair = 2 * rows
    there = pl.ds(pl.multiple_of(pair * q, LANES), pair)
    here = there if p is q else pl.ds(pair * p, pair)
    om, oq = outs[3], outs[0]
    half, nq = om.shape[1] // 2, oq.shape[0] // 2
    places = [(3, slice(second * half + skip, (second + 1) * half)), (key, slice(None))]
    places += [(0, slice(c * nq + second * nq // 2, c * nq + (second + 1) * nq // 2)) for c in range(CORES)]
    for a, cut in places:
        src = sources[a].at[here, cut] if a == 3 else sources[a].at[cut, here]
        dst = outs[a].at[there, cut] if a == 3 else outs[a].at[cut, there]
        pltpu.make_async_copy(src, dst, sem).start()


def publish_first(rows, *refs):
    at = Place()
    sources, outs, (token, done) = refs[:4], refs[4:8], refs[8:]
    token[...] = jnp.zeros_like(token)
    pair = 2 * rows
    oq, ok, _, om = sources
    units = unit_list(rows, om.shape[1], oq.shape[0] // 2, ok.shape[0] // 2)
    first = units[0][2]
    for key, second in ((1, 0), (2, 1)):
        put_list(rows, sources, at.chip, outs, at.chip, key, second, 0, done.at[0])
    put_list(rows, sources, at.chip_x, outs, at.chip_x, 1, 0, 0, done.at[1])
    put_list(rows, sources, at.chip_y, outs, at.chip_y, 2, 1, 0, done.at[1])
    block = pl.ds(pl.multiple_of(pair * at.chip_y, LANES), pair)
    pltpu.make_async_copy(om.at[block, :first], outs[3].at[block, :first], done.at[1]).start()
    lists = rows_of(units[: len(units) // 2])
    arrived(oq.at[: 4 * lists, :], done.at[0])
    arrived(oq.at[: 4 * lists + 2 * rows_of(units[:1]), :], done.at[1])


def publish_next(rows, *refs):
    at = Place()
    from_x, from_y, diag, norm = refs[:4], refs[4:8], refs[8:12], refs[12]
    *outs, norm_out, token, done = refs[17:]
    token[...] = jnp.zeros_like(token)
    oq, ok, _, om = outs
    units = unit_list(rows, om.shape[1], oq.shape[0] // 2, ok.shape[0] // 2)
    n = len(units) // 2
    put_list(rows, from_x, 0, outs, at.chip_x, 2, 1, 0, done.at[0])
    put_list(rows, from_y, 0, outs, at.chip_y, 1, 0, units[0][2], done.at[0])
    for j in range(BOTH):
        put_pair(units, j, rows, diag, outs, at.chip_d, done.at[1])
    pltpu.make_async_copy(norm, norm_out, done.at[2]).start()
    arrived(oq.at[: 4 * rows_of(units[:n]) - 2 * rows_of(units[:1]), :], done.at[0])
    arrived(oq.at[: 4 * rows_of(units[:BOTH]), :], done.at[1])
    arrived(norm, done.at[2])


def put_pair(units, j, rows, sources, outs, q, sem):
    for k in (j, len(units) // 2 + j):
        for core in range(CORES):
            src, dst = region(units[k], sources, rows, 0, core), region(units[k], outs, rows, q, core)
            pltpu.make_async_copy(src, dst, sem).start()


def publish_last(rows, *refs):
    at = Place()
    sources, outs, done = refs[:4], refs[8:12], refs[12]
    oq, ok, _, om = outs
    units = unit_list(rows, om.shape[1], oq.shape[0] // 2, ok.shape[0] // 2)
    n = len(units) // 2
    for j in range(BOTH, n):
        put_pair(units, j, rows, sources, outs, at.chip_d, done)
    arrived(oq.at[: 4 * rows_of(units[BOTH:n]), :], done)


def fast_body(zeros, widths, *args):
    tq, lq, hq, tk, lk, hk, tv, lv, hv, tm, lm, hm, nt, ns = args
    rows, depth = tq.shape[0], tq.shape[0] * zeros
    new = jax.ShapeDtypeStruct
    shapes = [(tq.shape[1], depth), (tk.shape[1], depth), (tv.shape[1], depth), (depth, tm.shape[0])]
    pair = 2 * rows
    held = 2 * sum(a * b for a, b in shapes)
    dma = pltpu.SemaphoreType.DMA
    count = len(unit_list(rows, tm.shape[0], tq.shape[1] // 2, tk.shape[1] // 2))
    moved = [tq, lq.T, hq, tk, lk.T, hk, tv, lv.T, hv, tm.T, lm.T, hm, nt[None, :], ns[None, :]]
    rank, mix = hm.shape[0], tm.shape[0]
    halves = (tq.shape[1] + tk.shape[1] + tv.shape[1]) // 2
    norms = (CORES, zeros // CORES, 1, LANES)
    in_vmem, in_hbm = pl.BlockSpec(memory_space=VMEM), pl.BlockSpec(memory_space=HBM)
    *most, on = pl.pallas_call(
        functools.partial(gather, zeros, widths),
        out_shape=[VMEM(s, BF16) for s in shapes] + [VMEM(norms, F32)],
        in_specs=[in_hbm] * len(args),
        out_specs=[in_vmem] * (len(shapes) + 1),
        scratch_shapes=[
            VMEM((rows, mix), BF16), VMEM((rank, mix + rows), BF16), VMEM((pair, halves), BF16),
            VMEM((3, 2, rank, rows), BF16), VMEM((rank, 2 * halves), BF16), VMEM((2, 1, nt.shape[0]), F32),
            VMEM((tq.shape[1] // 2, pair), BF16), VMEM((tk.shape[1] // 2, pair), BF16), VMEM((tv.shape[1] // 2, pair), BF16),
            VMEM((rows, mix), BF16), VMEM((rank, pair), BF16),
            dma((7,)), dma, dma((2,)), dma((2,)), dma, dma((count // 2 + 1,)), dma, dma, dma, dma, dma((3,)), dma((3,)),
        ],
        compiler_params=pltpu.CompilerParams(
            collective_id=0, has_side_effects=True, vmem_limit_bytes=VMEM_BYTES - held - 64 * 1024
        ),
        name="gather_merged",
    )(*moved)
    results = [new(s, BF16) for s in shapes]
    token = VMEM((8, LANES), F32)
    *done, went = pl.pallas_call(
        functools.partial(publish_first, rows),
        out_shape=results + [token],
        in_specs=[in_vmem] * 4,
        out_specs=[in_hbm] * 4 + [in_vmem],
        scratch_shapes=[dma((2,))],
        compiler_params=pltpu.CompilerParams(vmem_limit_bytes=2**20),
        name="publish_first",
    )(*most)
    part = [VMEM((s[0], pair), BF16) for s in shapes[:3]] + [VMEM((pair, shapes[3][1]), BF16)]
    *more, norm = pl.pallas_call(
        functools.partial(spread, zeros, widths),
        out_shape=part * 3 + [VMEM((depth,), BF16)],
        in_specs=[in_vmem] * 6,
        out_specs=[in_vmem] * 13,
        scratch_shapes=[
            VMEM((widths, *norms), F32), VMEM((1, depth), F32),
            pltpu.SemaphoreType.REGULAR, dma, dma, dma((count // 2,)), dma, dma((BOTH,)), dma, dma, dma, dma((2,)), dma((2,)),
        ],
        compiler_params=pltpu.CompilerParams(collective_id=1, has_side_effects=True, vmem_limit_bytes=2**20),
        name="spread",
    )(went, *most, on)
    *done, gain, went = pl.pallas_call(
        functools.partial(publish_next, rows),
        out_shape=results + [new((depth,), BF16), token],
        in_specs=[in_vmem] * 13 + [in_hbm] * 4,
        out_specs=[in_hbm] * 5 + [in_vmem],
        input_output_aliases={13 + k: k for k in range(4)},
        scratch_shapes=[dma((3,))],
        compiler_params=pltpu.CompilerParams(vmem_limit_bytes=2**20),
        name="publish_next",
    )(*more, norm, *done)
    rest = pl.pallas_call(
        finish,
        out_shape=part,
        in_specs=[in_vmem] * 9,
        out_specs=[in_vmem] * 4,
        scratch_shapes=[pltpu.SemaphoreType.REGULAR, dma, dma, dma((count // 2 - BOTH,)), dma, dma, dma],
        compiler_params=pltpu.CompilerParams(collective_id=2, has_side_effects=True, vmem_limit_bytes=2**20),
        name="finish",
    )(went, *most, *more[8:])
    full = pl.pallas_call(
        functools.partial(publish_last, rows),
        out_shape=results,
        in_specs=[in_vmem] * 4 + [in_hbm] * 4,
        out_specs=[in_hbm] * 4,
        input_output_aliases={4 + k: k for k in range(4)},
        scratch_shapes=[dma],
        compiler_params=pltpu.CompilerParams(vmem_limit_bytes=2**20),
        name="publish_last",
    )(*rest, *done)
    return (*full, gain)


def solution(mesh):
    placed = (
        P("zero", "width"), P("zero", None), P(None, "width"),
        P("zero", "width"), P("zero", None), P(None, "width"),
        P("zero", "width"), P("zero", None), P(None, "width"),
        P("width", "zero"), P("width", None), P(None, "zero"),
        P(("zero", "width")), P(("zero", "width")),
    )
    zeros, widths = mesh.shape["zero"], mesh.shape["width"]
    side = math.isqrt(zeros // CORES)

    def body(*args):
        rows, nq, nk, mix = args[0].shape[0], args[0].shape[1] // 2, args[3].shape[1] // 2, args[9].shape[0]
        square = side == 2 and CORES * side * side == zeros and args[6].shape == args[3].shape
        even = (2 * nq + 4 * nk) % mix == 0 and rows % 64 == 0
        if square and even and nq % 128 == 0 and nk % 128 == 0 and mix % (8 * LANES) == 0:
            return fast_body(zeros, widths, *args)
        return plain_body(*args)

    return jax.shard_map(
        body,
        mesh=mesh,
        in_specs=placed,
        out_specs=(P("width", None), P("width", None), P("width", None), P(None, "width"), P()),
        check_vma=False,
    )
```

```python
import functools
import math

import jax
import jax.numpy as jnp
from jax import lax
from jax.experimental import pallas as pl
from jax.experimental.pallas import tpu as pltpu
from jax.sharding import PartitionSpec as P

mix_rate = 0.5
CORES = 2
LANES = 128
F32 = jnp.float32
BF16 = jnp.bfloat16
AHEAD = 9
BOTH = 4
EARLY = 10
TWICE = 1
VMEM_BYTES = 67_043_328
VMEM = pltpu.VMEM
HBM = pltpu.MemorySpace.HBM


def plain_body(
    train_query, low_query, high_query, train_key, low_key, high_key, train_value, low_value, high_value,
    train_mixed, low_mixed, high_mixed, norm_train, norm_step,
):
    def merged(train, low, high):
        return (train.astype(F32) + mix_rate * jnp.dot(low, high, preferred_element_type=F32)).astype(BF16)

    return (
        lax.all_gather(merged(train_query, low_query, high_query), "zero", axis=0, tiled=True).T,
        lax.all_gather(merged(train_key, low_key, high_key), "zero", axis=0, tiled=True).T,
        lax.all_gather(merged(train_value, low_value, high_value), "zero", axis=0, tiled=True).T,
        lax.all_gather(merged(train_mixed, low_mixed, high_mixed).T, "zero", axis=0, tiled=True),
        lax.all_gather((norm_train + norm_step).astype(BF16), ("zero", "width"), axis=0, tiled=True),
    )


class Place:
    def __init__(self):
        self.me, self.w = lax.axis_index("zero"), lax.axis_index("width")
        me = self.me
        self.c = lax.rem(me, 2)
        x = lax.rem(lax.div(me, 2), 2)
        self.y = lax.div(me, 4)
        self.chip = lax.div(me, 2)
        self.partner, self.xn, self.yn = me + 1 - 2 * self.c, me + 2 - 4 * x, me + 4 - 8 * self.y
        self.chip_x, self.chip_y, self.chip_d = self.chip + 1 - 2 * x, self.chip + 2 - 4 * self.y, 3 - self.chip


def remote(src, dst, ssem, rsem, **where):
    return pltpu.make_async_remote_copy(
        src_ref=src, dst_ref=dst, send_sem=ssem, recv_sem=rsem, device_id=where, device_id_type=pl.DeviceIdType.MESH
    )


def tell(sem, **where):
    pl.semaphore_signal(sem, inc=1, device_id=where, device_id_type=pl.DeviceIdType.MESH)


def unit_list(rows, mix, nq, nk):
    eighth = mix // 8
    mixed = ((0, eighth), (eighth, 2 * eighth), (3 * eighth, eighth))
    query = ((0, nq // 8), (nq // 8, nq // 8), (nq // 4, nq // 4))
    parts = ((0, nk // 2), (nk // 2, nk // 4), (3 * nk // 4, nk // 8), (7 * nk // 8, nk // 8))
    return [
        (a, at + half, size)
        for key, share in ((1, 0), (2, 1))
        for a, half, pieces in ((3, share * mix // 2, mixed), (0, share * nq // 2, query), (key, 0, parts))
        for at, size in pieces
    ]


def region(unit, outs, rows, chip, c):
    a, start, size = unit
    out = outs[a]
    if a == 3:
        return out.at[pl.ds(pl.multiple_of(rows * (2 * chip + c), 16), rows), start : start + size]
    pair = 2 * rows
    return out.at[
        pl.ds(pl.multiple_of(c * (out.shape[0] // 2) + start, 16), size), pl.ds(pl.multiple_of(pair * chip, LANES), pair)
    ]


def arrived(ref, sem):
    pltpu.make_async_copy(ref, ref, sem).wait()


def gather(
    zeros, widths,
    tq_h, lq_h, hq_h, tk_h, lk_h, hk_h, tv_h, lv_h, hv_h, tm_h, lm_h, hm_h, nt_h, ns_h,
    oq, ok, ov, om, on,
    tm, pair_m, held, lows, highs, gains, own_q, own_k, own_v, own_m, joined,
    fetched, keep, swap_send, swap_recv, send, arrive, ahead_send, ahead_recv, cross_send, cross_recv, nsend, nrecv,
):
    at = Place()
    c, chip = at.c, at.chip
    rows = tq_h.shape[0]
    pair = 2 * rows
    mix = tm_h.shape[1]
    outs = (oq, ok, ov, om)
    nq, nk = oq.shape[0] // 2, ok.shape[0] // 2
    units = unit_list(rows, mix, nq, nk)
    n = len(units) // 2
    first = units[0][2]
    LOW_HIGH, FIRST, OTHERS, GAINS, LOWS, HIGHS, TRAINS = range(7)

    def rank_dot(left, right):
        return lax.dot_general(left, right, (((0,), (0,)), ((), ())), preferred_element_type=F32)

    def fetch(src, dst, sem):
        pltpu.make_async_copy(src, dst, fetched.at[sem]).start()

    barrier = pltpu.get_barrier_semaphore()
    for other in (at.xn, at.yn, at.partner):
        tell(barrier, zero=other)

    fetch(tm_h.at[:, :first], tm.at[:, :first], FIRST)
    fetch(hm_h, pair_m.at[:, mix:], LOW_HIGH)
    fetch(lm_h, pair_m.at[:, :mix], LOW_HIGH)
    fetch(nt_h, gains.at[0], GAINS)
    fetch(ns_h, gains.at[1], GAINS)
    fetch(tm_h.at[:, first:], tm.at[:, first:], OTHERS)

    mine = pl.ds(pl.multiple_of(rows * c, 16), rows)
    spans, spot = [], 0
    for train in (tq_h, tk_h, tv_h):
        spans.append(slice(spot, spot + train.shape[1] // 2))
        spot += train.shape[1] // 2
    for k, (train, low, high) in enumerate(((tq_h, lq_h, hq_h), (tk_h, lk_h, hk_h), (tv_h, lv_h, hv_h))):
        half = train.shape[1] // 2
        cols = pl.ds(pl.multiple_of(c * half, LANES), half)
        fetch(train.at[:, cols], held.at[mine, spans[k]], TRAINS)
        fetch(low, lows.at[k, c], LOWS)
        fetch(high, highs.at[:, 2 * spans[k].start : 2 * spans[k].stop], HIGHS)

    def merge_mixed(start, size):
        cols = slice(start, start + size)
        merged = tm[:, cols].astype(F32) + mix_rate * rank_dot(pair_m[:, mix:], pair_m[:, cols])
        own_m[:, cols] = merged.astype(BF16)

    sources = [
        own_m.at[:, s : s + size] if a == 3 else (own_q, own_k, own_v)[a].at[s : s + size, :] for a, s, size in units
    ]

    def link(k, along_x, ssem, rsem):
        there = region(units[k], outs, rows, chip, c)
        remote(sources[k], there, ssem, rsem, zero=at.xn if along_x else at.yn).start()

    def to_x(k):
        link(k, True, send, arrive.at[k])

    def to_y(k):
        link(k, False, send, arrive.at[k - n if k >= n else n])

    def cross(k, p):
        there = region(units[k], outs, rows, p, c)
        remote(sources[k] if p is chip else there, there, cross_send, cross_recv, zero=at.partner).start()

    arrived(pair_m, fetched.at[LOW_HIGH])
    arrived(tm.at[:, :first], fetched.at[FIRST])
    merge_mixed(0, first)

    pl.semaphore_wait(barrier, 3)
    to_x(0)
    to_y(0)
    for k, (train, low) in enumerate(((tq_h, lq_h), (tk_h, lk_h), (tv_h, lv_h))):
        half = train.shape[1] // 2
        cols = pl.ds(pl.multiple_of((1 - c) * half, LANES), half)
        remote(train.at[:, cols], held.at[mine, spans[k]], swap_send.at[0], swap_recv.at[0], zero=at.partner).start()
        remote(low, lows.at[k, c], swap_send.at[1], swap_recv.at[1], zero=at.partner).start()

    arrived(gains, fetched.at[GAINS])
    on[c, chip] = jnp.pad(gains[0] + gains[1], ((0, 0), (0, LANES - gains.shape[2])))
    arrived(tm.at[:, first:], fetched.at[OTHERS])
    for k in (n, 1, n + 1, 2, n + 2):
        merge_mixed(*units[k][1:])

    row = on.at[c, pl.ds(chip, 1)]
    both_rows = on.at[c, pl.ds(2 * at.y, 2)]
    small = [
        remote(row, row, nsend.at[0], nrecv.at[0], zero=at.xn),
        remote(both_rows, both_rows, nsend.at[1], nrecv.at[1], zero=at.yn),
        remote(on.at[c], on.at[c], nsend.at[2], nrecv.at[2], zero=at.partner),
    ]
    small[0].start()
    to_y(n)
    for j in (1, 2):
        to_x(j)
        to_y(n + j)

    def keep_own(source, there):
        pltpu.make_async_copy(source, there, keep).start()

    keep_own(own_m, om.at[pl.ds(pl.multiple_of(rows * at.me, 16), rows), :])

    def merge(e, out, own_out):
        span = spans[e]
        half = span.stop - span.start
        joined[:, :rows] = lows[e, 0]
        joined[:, rows:] = lows[e, 1]
        cols = pl.ds(pl.multiple_of(2 * span.start + c * half, LANES), half)
        for j in range(pair // LANES):
            part = slice(j * LANES, (j + 1) * LANES)
            merged = held[part, span].astype(F32) + mix_rate * rank_dot(joined[:, part], highs[:, cols])
            own_out[:, part] = merged.T.astype(BF16)
        keep_own(own_out, out.at[
            pl.ds(pl.multiple_of(c * half, 16), half), pl.ds(pl.multiple_of(pair * chip, LANES), pair)
        ])

    theirs = pl.ds(pl.multiple_of(rows * (1 - c), 16), rows)
    arrived(lows.at[:, 0], fetched.at[LOWS])
    arrived(highs, fetched.at[HIGHS])
    arrived(held.at[mine, :], fetched.at[TRAINS])
    arrived(lows.at[:, 0], swap_recv.at[1])
    arrived(held.at[theirs, :], swap_recv.at[0])
    merge(0, oq, own_q)
    small[0].wait()
    small[1].start()
    for j in (3, 4, 5):
        to_x(j)
        to_y(n + j)
    merge(1, ok, own_k)
    merge(2, ov, own_v)
    for j in range(6, n):
        to_x(j)
        to_y(n + j)
    @pl.when(c == 1)
    def _():
        for j in range(AHEAD):
            for k in second_pair(j, n):
                link(k, k >= n, ahead_send, ahead_recv)

    for k in range(2 * n):
        cross(k, chip)
    lists = rows_of(units[:n])
    for j in range(n):
        arrived(oq.at[: rows_of([units[j]] * 2), :], arrive.at[j])
        cross(j, at.chip_x)
        cross(n + j, at.chip_y)
        if j == 0:
            arrived(oq.at[: rows_of(units[:1]), :], arrive.at[n])
            cross(0, at.chip_y)
        if j == n - 4:
            small[1].wait()
            small[2].start()
    arrived(lows.at[:, 0], swap_send.at[1])
    arrived(held.at[mine, :], swap_send.at[0])
    arrived(oq.at[: 2 * lists, :], keep)
    small[2].wait()
    phase = oq.at[: 2 * lists + rows_of(units[:1]), :]
    arrived(phase, send)
    arrived(oq.at[: 4 * lists + rows_of(units[:1]), :], cross_send)
    arrived(oq.at[: 4 * lists + rows_of(units[:1]), :], cross_recv)

    @pl.when(c == 1)
    def _():
        ahead = oq.at[: rows_of([units[k] for j in range(AHEAD) for k in second_pair(j, n)]), :]
        arrived(ahead, ahead_send)
        arrived(ahead, ahead_recv)


def second_pair(j, n):
    return (n + j, j) if j else (n,)


def rows_of(units):
    return sum(size // 8 if a == 3 else size // 4 for a, _, size in units)


def enter(at, z_peers, ready, told):
    c = at.c
    barrier = pltpu.get_barrier_semaphore()
    for other in (at.xn, at.yn):
        tell(barrier, zero=other)

    @pl.when(c == 1)
    def _():
        for w in z_peers:
            tell(barrier, width=w)

    pl.semaphore_wait(barrier, 2 + (1 + len(z_peers)) * c)
    pl.when(c == 0)(lambda: tell(barrier, zero=at.partner))

    @pl.when(c == 1)
    def _():
        for other in told:
            tell(ready, zero=other)


def spread(zeros, widths, *refs):
    (
        _, oq, ok, ov, om, on, xq, xk, xv, xm, yq, yk, yv, ym, dq, dk, dv, dm, norm,
        every, flat, ready, copied, send, arrive, on_send, on_recv, early_recv, cross_send, cross_recv, nsend, nrecv,
    ) = refs
    at = Place()
    c = at.c
    outs, from_x, from_y, diag = (oq, ok, ov, om), (xq, xk, xv, xm), (yq, yk, yv, ym), (dq, dk, dv, dm)
    rows = dm.shape[0] // 2
    units = unit_list(rows, om.shape[1], oq.shape[0] // 2, ok.shape[0] // 2)
    n = len(units) // 2
    z_peers = [lax.rem(at.w + d, widths) for d in range(1, widths)]
    enter(at, z_peers, ready, [at.partner])

    def own(j):
        for k in second_pair(j, n):
            source = region(units[k], outs, rows, at.chip, c)
            there = region(units[k], from_x if k >= n else from_y, rows, 0, c)
            remote(source, there, send, arrive.at[j], zero=at.xn if k >= n else at.yn).start()

    def onward(j):
        for k in (j, n + j):
            source = region(units[k], outs, rows, at.chip_x if k < n else at.chip_y, c)
            there = region(units[k], diag, rows, 0, c)
            recv = on_recv.at[j] if j < BOTH else early_recv
            remote(source, there, on_send, recv, zero=at.yn if k < n else at.xn).start()

    def across(j, ahead):
        for k in second_pair(j, n):
            there = region(units[k], from_x if k >= n else from_y, rows, 0, c)
            source = region(units[k], outs, rows, at.chip_x if k >= n else at.chip_y, c) if ahead else there
            remote(source, there, cross_send, cross_recv, zero=at.partner).start()
            if ahead:
                pltpu.make_async_copy(source, there, copied).start()

    def some(core_0_alone, step):
        pl.when(c == 0)(step) if core_0_alone else step()

    def send_all(first, pairs):
        for j in range(first, n):
            own(j)
        for j in range(pairs):
            onward(j)

    pl.when(c == 0)(lambda: send_all(0, BOTH))
    to_partner = remote(every, every, nsend.at[0], nrecv.at[0], zero=at.partner)

    @pl.when(c == 1)
    def _():
        for w in z_peers:
            remote(on, every.at[at.w], nsend.at[1], nrecv.at[1], width=w).start()
        for j in range(AHEAD):
            across(j, True)
        every[at.w] = on[...]
        for sems in (nsend, nrecv):
            arrived(every.at[: widths - 1], sems.at[1])
        send_all(AHEAD, EARLY)
        to_partner.start()

    pl.when(c == 0)(lambda: pl.semaphore_wait(ready, 1))
    for j in range(n):

        def pass_on():
            arrived(oq.at[: rows_of([units[k] for k in second_pair(j, n)]), :], arrive.at[j])
            across(j, False)

        some(j < AHEAD, pass_on)
    size = norm.shape[0] // (zeros * widths)
    pl.when(c == 0)(lambda: to_partner.wait_recv())
    for zero in range(zeros):
        for w in range(widths):
            i = zero * widths + w
            flat[:, i * size : (i + 1) * size] = every[w, zero % 2, zero // 2][:, :size]
    norm[...] = flat[0, :].astype(BF16)
    for j in range(BOTH):
        arrived(oq.at[: 2 * rows_of(units[j : j + 1]), :], on_recv.at[j])
        for k in (j, n + j):
            there = region(units[k], diag, rows, 0, c)
            remote(there, there, cross_send, cross_recv, zero=at.partner).start()

    second = rows_of([units[k] for j in range(n) for k in second_pair(j, n)])
    ahead = rows_of([units[k] for j in range(AHEAD) for k in second_pair(j, n)])
    common, early = 2 * rows_of(units[:BOTH]), 2 * rows_of(units[:EARLY])

    @pl.when(c == 0)
    def _():
        arrived(oq.at[:second, :], send)
        arrived(oq.at[:common, :], on_send)

    arrived(oq.at[: second + common, :], cross_send)
    arrived(oq.at[: second + common, :], cross_recv)

    @pl.when(c == 1)
    def _():
        to_partner.wait_send()
        arrived(oq.at[:ahead, :], copied)
        if AHEAD < n:
            arrived(oq.at[: second - ahead, :], send)
        arrived(oq.at[:early, :], on_send)
        arrived(oq.at[: early - common, :], early_recv)


def finish(*refs):
    _, oq, ok, ov, om, dq, dk, dv, dm, rq, rk, rv, rm, ready, copied, on_send, on_recv, send, recv, last_recv = refs
    at = Place()
    c = at.c
    outs, held, diag = (oq, ok, ov, om), (dq, dk, dv, dm), (rq, rk, rv, rm)
    rows = rm.shape[0] // 2
    units = unit_list(rows, om.shape[1], oq.shape[0] // 2, ok.shape[0] // 2)
    n = len(units) // 2
    common, once, whole = (2 * rows_of(units[:count]) for count in (BOTH, n - TWICE, n))
    other_x, other_y = at.xn + at.partner - at.me, at.yn + at.partner - at.me
    enter(at, [], ready, [at.partner, other_x, other_y])

    def onward(j, other=False):
        for k in (j, n + j):
            source = region(units[k], outs, rows, at.chip_x if k < n else at.chip_y, c)
            there = region(units[k], diag, rows, 0, c)
            where = (other_y if k < n else other_x) if other else (at.yn if k < n else at.xn)
            remote(source, there, on_send, last_recv if other else on_recv.at[j - BOTH], zero=where).start()

    def across(j, early):
        for k in (j, n + j):
            there = region(units[k], diag, rows, 0, c)
            source = region(units[k], held, rows, 0, c) if early else there
            remote(source, there, send, recv, zero=at.partner).start()
            if early:
                pltpu.make_async_copy(source, there, copied).start()

    @pl.when(c == 1)
    def _():
        for j in range(BOTH, n):
            across(j, True)
        arrived(oq.at[: whole - common, :], copied)
        arrived(oq.at[: whole - common, :], send)
        arrived(oq.at[: whole - once, :], last_recv)
        arrived(oq.at[: once - common, :], recv)

    @pl.when(c == 0)
    def _():
        for j in range(BOTH, n):
            onward(j)
        pl.semaphore_wait(ready, 3)
        for j in range(n - TWICE, n):
            onward(j, True)
        for j in range(BOTH, n):
            arrived(oq.at[: 2 * rows_of(units[j : j + 1]), :], on_recv.at[j - BOTH])
            if j < n - TWICE:
                across(j, False)
        arrived(oq.at[: whole - common + whole - once, :], on_send)
        arrived(oq.at[: once - common, :], send)
        arrived(oq.at[: whole - common, :], recv)


def put_list(rows, sources, p, outs, q, key, second, skip, sem):
    pair = 2 * rows
    there = pl.ds(pl.multiple_of(pair * q, LANES), pair)
    here = there if p is q else pl.ds(pair * p, pair)
    om, oq = outs[3], outs[0]
    half, nq = om.shape[1] // 2, oq.shape[0] // 2
    places = [(3, slice(second * half + skip, (second + 1) * half)), (key, slice(None))]
    places += [(0, slice(c * nq + second * nq // 2, c * nq + (second + 1) * nq // 2)) for c in range(CORES)]
    for a, cut in places:
        src = sources[a].at[here, cut] if a == 3 else sources[a].at[cut, here]
        dst = outs[a].at[there, cut] if a == 3 else outs[a].at[cut, there]
        pltpu.make_async_copy(src, dst, sem).start()


def publish_first(rows, *refs):
    at = Place()
    sources, outs, (token, done) = refs[:4], refs[4:8], refs[8:]
    token[...] = jnp.zeros_like(token)
    pair = 2 * rows
    oq, ok, _, om = sources
    units = unit_list(rows, om.shape[1], oq.shape[0] // 2, ok.shape[0] // 2)
    first = units[0][2]
    for key, second in ((1, 0), (2, 1)):
        put_list(rows, sources, at.chip, outs, at.chip, key, second, 0, done.at[0])
    put_list(rows, sources, at.chip_x, outs, at.chip_x, 1, 0, 0, done.at[1])
    put_list(rows, sources, at.chip_y, outs, at.chip_y, 2, 1, 0, done.at[1])
    block = pl.ds(pl.multiple_of(pair * at.chip_y, LANES), pair)
    pltpu.make_async_copy(om.at[block, :first], outs[3].at[block, :first], done.at[1]).start()
    lists = rows_of(units[: len(units) // 2])
    arrived(oq.at[: 4 * lists, :], done.at[0])
    arrived(oq.at[: 4 * lists + 2 * rows_of(units[:1]), :], done.at[1])


def publish_next(rows, *refs):
    at = Place()
    from_x, from_y, diag, norm = refs[:4], refs[4:8], refs[8:12], refs[12]
    *outs, norm_out, token, done = refs[17:]
    token[...] = jnp.zeros_like(token)
    oq, ok, _, om = outs
    units = unit_list(rows, om.shape[1], oq.shape[0] // 2, ok.shape[0] // 2)
    n = len(units) // 2
    put_list(rows, from_x, 0, outs, at.chip_x, 2, 1, 0, done.at[0])
    put_list(rows, from_y, 0, outs, at.chip_y, 1, 0, units[0][2], done.at[0])
    for j in range(BOTH):
        put_pair(units, j, rows, diag, outs, at.chip_d, done.at[1])
    pltpu.make_async_copy(norm, norm_out, done.at[2]).start()
    arrived(oq.at[: 4 * rows_of(units[:n]) - 2 * rows_of(units[:1]), :], done.at[0])
    arrived(oq.at[: 4 * rows_of(units[:BOTH]), :], done.at[1])
    arrived(norm, done.at[2])


def put_pair(units, j, rows, sources, outs, q, sem):
    for k in (j, len(units) // 2 + j):
        for core in range(CORES):
            src, dst = region(units[k], sources, rows, 0, core), region(units[k], outs, rows, q, core)
            pltpu.make_async_copy(src, dst, sem).start()


def publish_last(rows, *refs):
    at = Place()
    sources, outs, done = refs[:4], refs[8:12], refs[12]
    oq, ok, _, om = outs
    units = unit_list(rows, om.shape[1], oq.shape[0] // 2, ok.shape[0] // 2)
    n = len(units) // 2
    for j in range(BOTH, n):
        put_pair(units, j, rows, sources, outs, at.chip_d, done)
    arrived(oq.at[: 4 * rows_of(units[BOTH:n]), :], done)


def fast_body(zeros, widths, *args):
    tq, lq, hq, tk, lk, hk, tv, lv, hv, tm, lm, hm, nt, ns = args
    rows, depth = tq.shape[0], tq.shape[0] * zeros
    new = jax.ShapeDtypeStruct
    shapes = [(tq.shape[1], depth), (tk.shape[1], depth), (tv.shape[1], depth), (depth, tm.shape[0])]
    pair = 2 * rows
    held = 2 * sum(a * b for a, b in shapes)
    dma = pltpu.SemaphoreType.DMA
    count = len(unit_list(rows, tm.shape[0], tq.shape[1] // 2, tk.shape[1] // 2))
    moved = [tq, lq.T, hq, tk, lk.T, hk, tv, lv.T, hv, tm.T, lm.T, hm, nt[None, :], ns[None, :]]
    rank, mix = hm.shape[0], tm.shape[0]
    halves = (tq.shape[1] + tk.shape[1] + tv.shape[1]) // 2
    norms = (CORES, zeros // CORES, 1, LANES)
    in_vmem, in_hbm = pl.BlockSpec(memory_space=VMEM), pl.BlockSpec(memory_space=HBM)
    *most, on = pl.pallas_call(
        functools.partial(gather, zeros, widths),
        out_shape=[VMEM(s, BF16) for s in shapes] + [VMEM(norms, F32)],
        in_specs=[in_hbm] * len(args),
        out_specs=[in_vmem] * (len(shapes) + 1),
        scratch_shapes=[
            VMEM((rows, mix), BF16), VMEM((rank, mix + rows), BF16), VMEM((pair, halves), BF16),
            VMEM((3, 2, rank, rows), BF16), VMEM((rank, 2 * halves), BF16), VMEM((2, 1, nt.shape[0]), F32),
            VMEM((tq.shape[1] // 2, pair), BF16), VMEM((tk.shape[1] // 2, pair), BF16), VMEM((tv.shape[1] // 2, pair), BF16),
            VMEM((rows, mix), BF16), VMEM((rank, pair), BF16),
            dma((7,)), dma, dma((2,)), dma((2,)), dma, dma((count // 2 + 1,)), dma, dma, dma, dma, dma((3,)), dma((3,)),
        ],
        compiler_params=pltpu.CompilerParams(
            collective_id=0, has_side_effects=True, vmem_limit_bytes=VMEM_BYTES - held - 64 * 1024
        ),
        name="gather_merged",
    )(*moved)
    results = [new(s, BF16) for s in shapes]
    token = VMEM((8, LANES), F32)
    *done, went = pl.pallas_call(
        functools.partial(publish_first, rows),
        out_shape=results + [token],
        in_specs=[in_vmem] * 4,
        out_specs=[in_hbm] * 4 + [in_vmem],
        scratch_shapes=[dma((2,))],
        compiler_params=pltpu.CompilerParams(vmem_limit_bytes=2**20),
        name="publish_first",
    )(*most)
    part = [VMEM((s[0], pair), BF16) for s in shapes[:3]] + [VMEM((pair, shapes[3][1]), BF16)]
    *more, norm = pl.pallas_call(
        functools.partial(spread, zeros, widths),
        out_shape=part * 3 + [VMEM((depth,), BF16)],
        in_specs=[in_vmem] * 6,
        out_specs=[in_vmem] * 13,
        scratch_shapes=[
            VMEM((widths, *norms), F32), VMEM((1, depth), F32),
            pltpu.SemaphoreType.REGULAR, dma, dma, dma((count // 2,)), dma, dma((BOTH,)), dma, dma, dma, dma((2,)), dma((2,)),
        ],
        compiler_params=pltpu.CompilerParams(collective_id=1, has_side_effects=True, vmem_limit_bytes=2**20),
        name="spread",
    )(went, *most, on)
    *done, gain, went = pl.pallas_call(
        functools.partial(publish_next, rows),
        out_shape=results + [new((depth,), BF16), token],
        in_specs=[in_vmem] * 13 + [in_hbm] * 4,
        out_specs=[in_hbm] * 5 + [in_vmem],
        input_output_aliases={13 + k: k for k in range(4)},
        scratch_shapes=[dma((3,))],
        compiler_params=pltpu.CompilerParams(vmem_limit_bytes=2**20),
        name="publish_next",
    )(*more, norm, *done)
    rest = pl.pallas_call(
        finish,
        out_shape=part,
        in_specs=[in_vmem] * 9,
        out_specs=[in_vmem] * 4,
        scratch_shapes=[pltpu.SemaphoreType.REGULAR, dma, dma, dma((count // 2 - BOTH,)), dma, dma, dma],
        compiler_params=pltpu.CompilerParams(collective_id=2, has_side_effects=True, vmem_limit_bytes=2**20),
        name="finish",
    )(went, *most, *more[8:])
    full = pl.pallas_call(
        functools.partial(publish_last, rows),
        out_shape=results,
        in_specs=[in_vmem] * 4 + [in_hbm] * 4,
        out_specs=[in_hbm] * 4,
        input_output_aliases={4 + k: k for k in range(4)},
        scratch_shapes=[dma],
        compiler_params=pltpu.CompilerParams(vmem_limit_bytes=2**20),
        name="publish_last",
    )(*rest, *done)
    return (*full, gain)


def solution(mesh):
    placed = (
        P("zero", "width"), P("zero", None), P(None, "width"),
        P("zero", "width"), P("zero", None), P(None, "width"),
        P("zero", "width"), P("zero", None), P(None, "width"),
        P("width", "zero"), P("width", None), P(None, "zero"),
        P(("zero", "width")), P(("zero", "width")),
    )
    zeros, widths = mesh.shape["zero"], mesh.shape["width"]
    side = math.isqrt(zeros // CORES)

    def body(*args):
        rows, nq, nk, mix = args[0].shape[0], args[0].shape[1] // 2, args[3].shape[1] // 2, args[9].shape[0]
        square = side == 2 and CORES * side * side == zeros and args[6].shape == args[3].shape
        even = (2 * nq + 4 * nk) % mix == 0 and rows % 64 == 0
        if square and even and nq % 128 == 0 and nk % 128 == 0 and mix % (8 * LANES) == 0:
            return fast_body(zeros, widths, *args)
        return plain_body(*args)

    return jax.shard_map(
        body,
        mesh=mesh,
        in_specs=placed,
        out_specs=(P("width", None), P("width", None), P("width", None), P(None, "width"), P()),
        check_vma=False,
    )
```
